32 devices in a mesh: rows: 2 (over y), cols: 4 (over z), slabs: 2 (over x), trial: 2 (over core).
Axes of the slice: x: 2, y: 2, z: 4, core: 2. Of those that a mesh axis runs over, the one named last changes fastest.
Arguments:
- field_values: float32 [64, 16, 256, 128], P(('trial', 'rows'), 'cols', 'slabs'), parts along dimension 0, may hold values from 0.5 to 2
- conductance: float32 [64, 16, 256, 128], P(('trial', 'rows'), 'cols', 'slabs'), parts along dimension 0, may hold values from 0.03 to 0.15
- source: float32 [64, 16, 256, 128], P(('trial', 'rows'), 'cols', 'slabs'), parts along dimension 0, may hold values from -0.2 to 0.2
Outputs:
- anomaly: float32 [64, 16, 256, 128], P(('trial', 'rows'), 'cols', 'slabs'), parts along dimension 0
- field_values_end: float32 [64, 16, 256, 128], P(('trial', 'rows'), 'cols', 'slabs'), parts along dimension 0
The draws below stay inside these ranges and needn't reach their ends.
There are 2 independent parts, one for each index of `trial`. The reference program is written for one: setup_inputs(seed, part) draws one part's arguments, and reference() takes and returns one part's arrays. A program takes and returns all parts, laid end to end along the dimension named above; each array names one. Nothing has to cross between parts.
All inputs are finite; a program needn't handle non-finite values.
Results may differ from the reference program's by a relative error of at most 0.00002.
Values sent between devices are 32-bit elements; how exact they have to be, the bound alone decides.
No kernel may reach another device: no remote copies, remote signals or barrier semaphores. Data moves between devices by JAX's collectives and lax.ppermute only.
A program may use at most 128 MiB of HBM per device.

```python
import jax
import jax.numpy as jnp
from jax import lax

GRID_J = 32
GRID_I = 16
GRID_K = 256
LEVELS = 128
STEPS = 4


def steps_of(own_key, extent, split, least, largest):
    factor_of, own = 1.0, jax.random.fold_in(own_key, 6)
    for dim, shards_of in split:
        draws = jnp.exp(jax.random.uniform(jax.random.fold_in(own, dim), (shards_of,), jnp.float32, least / len(split), largest / len(split)))
        factor_of = factor_of * jnp.repeat(draws, extent[dim] // shards_of).reshape([-1 if axis == dim else 1 for axis in range(len(extent))])
    return factor_of


def setup_inputs(seed: int = 0, part: int = 0) -> dict:
    keys = jax.random.split(jax.random.key(seed), 4)
    part_splits = jax.random.split(jax.random.fold_in(keys[3], part), 4)
    field_values = jnp.clip(0.5 + 1.5 * jax.random.uniform(part_splits[0], (GRID_J, GRID_I, GRID_K, LEVELS), jnp.float32) ** steps_of(part_splits[0], (GRID_J, GRID_I, GRID_K, LEVELS), ((0, 2), (1, 4), (2, 2)), -0.2, 0.2), 0.5, 2.0)
    conductance = jnp.clip(0.03 + 0.120000007 * jax.random.uniform(part_splits[1], (GRID_J, GRID_I, GRID_K, LEVELS), jnp.float32) ** steps_of(part_splits[1], (GRID_J, GRID_I, GRID_K, LEVELS), ((0, 2), (1, 4), (2, 2)), -0.2, 0.2), 0.03, 0.15)
    source = jnp.clip(jax.random.uniform(part_splits[2], (GRID_J, GRID_I, GRID_K, LEVELS), jnp.float32, -0.2, 0.2) * steps_of(part_splits[2], (GRID_J, GRID_I, GRID_K, LEVELS), ((0, 2), (1, 4), (2, 2)), -0.4, 0.0), -0.2, 0.2)
    return dict(field_values=field_values, conductance=conductance, source=source)


def strip_edges(values, dims):
    for dim in dims:
        values = lax.slice_in_dim(values, 1, values.shape[dim] - 1, axis=dim)
    return values

def neighbour(values, dim, start, dims):
    others = [other for other in dims if other != dim]
    values = strip_edges(values, others)
    return lax.slice_in_dim(values, start, start + values.shape[dim] - 2, axis=dim)

def one_step(padded, conductance, source):
    middle = strip_edges(padded, (0, 1, 2))
    lower = [neighbour(padded, dim, 0, (0, 1, 2)) for dim in (0, 1, 2)]
    upper = [neighbour(padded, dim, 2, (0, 1, 2)) for dim in (0, 1, 2)]
    spread = lower[0] + upper[0] + lower[1] + upper[1] + lower[2] + upper[2] - 6.0 * middle
    return middle + conductance * spread + source

def reference(field_values, conductance, source):
    for step in range(STEPS):
        field_values = one_step(jnp.pad(field_values, ((1, 1), (1, 1), (1, 1), (0, 0)), mode='constant'), conductance, source)
    line_mean = lax.optimization_barrier(jnp.mean(field_values, axis=0, keepdims=True))
    centred = field_values - line_mean
    line_variance = lax.optimization_barrier(jnp.mean(centred * centred, axis=0, keepdims=True))
    anomaly = centred * lax.rsqrt(line_variance + 0.0001)
    return (anomaly, field_values)
```

```python
import jax
import jax.numpy as jnp
from jax import lax
from jax.experimental import pallas as pl
from jax.experimental.pallas import tpu as pltpu
from jax.sharding import PartitionSpec as P

STEPS = 4
CHUNKS = 2
ROWS = 8
HBM = pl.BlockSpec(memory_space=pltpu.HBM)
VMEM = pl.BlockSpec(memory_space=pltpu.VMEM)
F32 = jnp.float32


def vmem(*shape):
    return pltpu.VMEM(shape, F32)


def call(body, ins, in_specs, outs, out_specs, name, scratch=(), aliases=None, flops=0):
    return pl.pallas_call(
        body,
        in_specs=in_specs,
        out_shape=outs,
        out_specs=out_specs,
        scratch_shapes=scratch,
        input_output_aliases=aliases or {},
        compiler_params=pltpu.CompilerParams(vmem_limit_bytes=12 * 2**20),
        cost_estimate=pl.CostEstimate(flops=flops, bytes_accessed=0, transcendentals=0) if flops else None,
        name=name,
    )(*ins)


def ports_of(axis):
    return ("swap",) if lax.axis_size(axis) == 2 else ("up", "down")


def exchange(buffers, axis, ports=None):
    count = lax.axis_size(axis)
    perms = {
        "swap": [(0, 1), (1, 0)],
        "up": [(i, i + 1) for i in range(count - 1)],
        "down": [(i + 1, i) for i in range(count - 1)],
    }
    return [lax.ppermute(buffer, axis, perms[port]) for buffer, port in zip(buffers, ports or ports_of(axis))]


def sent_index(axis, port, extent):
    if port == "swap":
        return (1 - lax.axis_index(axis)) * (extent - 1)
    return extent - 1 if port == "up" else 0


def halo_readers(axis, refs):
    if len(refs) == 1:
        at = lax.axis_index(axis)
        has_lower = at.astype(F32)
        has_upper = (1 - at).astype(F32)
        return (lambda where: refs[0][where] * has_lower), (lambda where: refs[0][where] * has_upper)
    return (lambda where: refs[0][where]), (lambda where: refs[1][where])


def run_copies(copies):
    for copy in copies:
        copy.start()
    for copy in copies:
        copy.wait()


def first_faces(field, spans):
    J, I, K, L = field.shape
    y_ports, x_ports = ports_of("rows"), ports_of("slabs")

    def body(u, *refs):
        outs, sems = refs[:-1], refs[-1]
        outs = list(outs)
        pairs = []
        for k0, kc in spans:
            pairs.append((u.at[:, I - 1, pl.ds(k0, kc)], outs.pop(0)))
            pairs.append((u.at[:, 0, pl.ds(k0, kc)], outs.pop(0)))
        for k0, kc in spans:
            for port in y_ports:
                pairs.append((u.at[sent_index("rows", port, J), :, pl.ds(k0, kc)], outs.pop(0)))
        for port in x_ports:
            pairs.append((u.at[:, :, sent_index("slabs", port, K)], outs.pop(0)))
        run_copies([pltpu.make_async_copy(src, dst, sems.at[n]) for n, (src, dst) in enumerate(pairs)])

    shapes = []
    for _, kc in spans:
        shapes += [vmem(J, kc, L)] * 2
    for _, kc in spans:
        shapes += [vmem(I, kc, L)] * len(y_ports)
    shapes += [vmem(J, I, L)] * len(x_ports)
    outs = list(
        call(body, [field], [HBM], shapes, [VMEM] * len(shapes), "first_faces", [pltpu.SemaphoreType.DMA((len(shapes),))])
    )
    z = [[outs.pop(0), outs.pop(0)] for _ in spans]
    y = [[outs.pop(0) for _ in y_ports] for _ in spans]
    return z, y, outs


def load(arrays, spans):
    J, I, K, L = arrays[0].shape

    def body(*refs):
        ins, outs, sems = refs[: len(arrays)], refs[len(arrays) : -1], refs[-1]
        copies = []
        for n, ref in enumerate(ins):
            for m, (k0, kc) in enumerate(spans):
                at = n * len(spans) + m
                copies.append(pltpu.make_async_copy(ref.at[:, :, pl.ds(k0, kc)], outs[at], sems.at[at]))
        run_copies(copies)

    shapes = [vmem(J, I, kc, L) for _ in arrays for _, kc in spans]
    outs = call(
        body, arrays, [HBM] * len(arrays), shapes, [VMEM] * len(shapes), "load", [pltpu.SemaphoreType.DMA((len(shapes),))]
    )
    return [outs[n * len(spans) : (n + 1) * len(spans)] for n in range(len(arrays))]


def step(q, fields, cond, src, z_in, y_in, x_in, layers, last, newer):
    J, I, kc, L = fields[q].shape
    n_chunks = len(fields)
    z_in = z_in if z_in is not None else []
    y_ports, x_ports = ports_of("rows"), ports_of("slabs")
    send_x = not last and q == n_chunks - 1
    below = fields[q - 1] if q > 0 else None
    above = fields[q + 1] if q + 1 < n_chunks else None
    ins = [fields[q], cond, src] + [a for a in (below, above) if a is not None] + list(z_in) + list(y_in) + list(x_in)
    if send_x:
        ins.append(newer)
    nl = len(layers)

    def body(*refs):
        refs = list(refs)
        u, c, s = refs.pop(0), refs.pop(0), refs.pop(0)
        lower_u = refs.pop(0) if below is not None else None
        upper_u = refs.pop(0) if above is not None else None
        z = [refs.pop(0) for _ in z_in]
        y = [refs.pop(0) for _ in y_in]
        x = [refs.pop(0) for _ in x_in]
        first_u = refs.pop(0) if send_x else None
        out = refs.pop(0)
        y_lo, y_hi = halo_readers("rows", y)
        x_lo, x_hi = halo_readers("slabs", x)
        sublane = lax.broadcasted_iota(jnp.int32, (ROWS, L), 0)

        def tile(k, at_low, at_high):
            here = pl.ds(k, ROWS)
            known = {}

            def cells(j, i):
                if (j, i) not in known:
                    if j < 0:
                        known[j, i] = y_lo((i, here))
                    elif j >= J:
                        known[j, i] = y_hi((i, here))
                    elif i < 0:
                        known[j, i] = z[0][j, here]
                    elif i >= I:
                        known[j, i] = z[1][j, here]
                    else:
                        known[j, i] = u[j, i, here]
                return known[j, i]

            def edge_row(ref, j, i, row):
                return jnp.broadcast_to(ref[j, i, pl.ds(row, 1)], (ROWS, L))

            def k_lower(j, i):
                if not at_low:
                    return u[j, i, pl.ds(k - 1, ROWS)]
                if lower_u is not None:
                    edge = edge_row(lower_u, j, i, lower_u.shape[2] - 1)
                else:
                    edge = jnp.broadcast_to(x_lo((j, pl.ds(i, 1))), (ROWS, L))
                return jnp.where(sublane == 0, edge, pltpu.roll(cells(j, i), 1, 0))

            def k_upper(j, i):
                if not at_high:
                    return u[j, i, pl.ds(k + 1, ROWS)]
                if upper_u is not None:
                    edge = edge_row(upper_u, j, i, 0)
                else:
                    edge = jnp.broadcast_to(x_hi((j, pl.ds(i, 1))), (ROWS, L))
                return jnp.where(sublane == ROWS - 1, edge, pltpu.roll(cells(j, i), ROWS - 1, 0))

            totals = [None] * nl
            for j in range(J):
                for n, i in enumerate(layers):
                    middle = cells(j, i)
                    spread = (
                        (cells(j - 1, i) + cells(j + 1, i))
                        + (cells(j, i - 1) + cells(j, i + 1))
                        + (k_lower(j, i) + k_upper(j, i))
                        - 6.0 * middle
                    )
                    new = middle + c[j, i, here] * spread + s[j, i, here]
                    out[j, n, here] = new
                    if last:
                        totals[n] = new if j == 0 else totals[n] + new
                    else:
                        if i == I - 1:
                            z_up[j, here] = new
                        if i == 0:
                            z_down[j, here] = new
                for i in list(known):
                    if i[0] < j:
                        del known[i]
            if last:
                for n in range(nl):
                    mean = totals[n] * (1.0 / J)
                    spread = None
                    for j in range(J):
                        off = out[j, n, here] - mean
                        spread = off * off if j == 0 else spread + off * off
                    stats[0, n, here] = mean
                    stats[1, n, here] = spread

        if last:
            stats = refs.pop(0)
        else:
            z_up, z_down = refs.pop(0), refs.pop(0)
            y_out = [refs.pop(0) for _ in y_ports]
            x_out = [refs.pop(0) for _ in x_ports] if send_x else []

        tiles = kc // ROWS
        tile(0, True, tiles == 1)
        if tiles > 2:

            def inner(t, carry):
                tile(pl.multiple_of(t * ROWS, ROWS), False, False)
                return carry

            lax.fori_loop(1, tiles - 1, inner, 0)
        if tiles > 1:
            tile(kc - ROWS, False, True)
        if not last:
            for ref, port in zip(y_out, y_ports):
                ref[...] = out[sent_index("rows", port, J)]
            for ref, port in zip(x_out, x_ports):
                for j in range(J):
                    head = first_u[j, :, 0, :]
                    tail = out[j, :, kc - 1, :]
                    if port == "swap":
                        at = lax.axis_index("slabs").astype(F32)
                        ref[j] = head * at + tail * (1.0 - at)
                    else:
                        ref[j] = tail if port == "up" else head

    shapes = [vmem(J, nl, kc, L)]
    if last:
        shapes.append(vmem(2, nl, kc, L))
    else:
        shapes += [vmem(J, kc, L)] * 2 + [vmem(I, kc, L)] * len(y_ports)
        if send_x:
            shapes += [vmem(J, I, L)] * len(x_ports)
    outs = list(
        call(
            body,
            ins,
            [VMEM] * len(ins),
            shapes,
            [VMEM] * len(shapes),
            f"step_{'last' if last else 'mid'}_{q}_{'_'.join(map(str, layers))}",
            flops=10 * J * nl * kc * L,
        )
    )
    new = outs.pop(0)
    if last:
        return new, outs[0]
    z = [outs.pop(0), outs.pop(0)]
    y = [outs.pop(0) for _ in y_ports]
    return new, z, y, outs


def finish(new, own, others, layers, span, buffers, shape):
    J, I, K, L = shape
    k0, kc = span
    nl = len(layers)
    count = len(others) + 1

    def body(*refs):
        refs = list(refs)
        u = refs.pop(0)
        sums = [refs.pop(0) for _ in range(count)]
        if buffers:
            refs.pop(0), refs.pop(0)
        anomaly_out, field_out, scaled, sems = refs
        copies = []
        for n, i in enumerate(layers):
            copies.append(pltpu.make_async_copy(u.at[:, n], field_out.at[:, i, pl.ds(k0, kc)], sems.at[n]))
            copies[-1].start()

        for n, i in enumerate(layers):

            def tile(t, carry):
                here = pl.ds(pl.multiple_of(t * ROWS, ROWS), ROWS)
                means = [ref[0, n, here] for ref in sums]
                mean = means[0]
                for other in means[1:]:
                    mean = mean + other
                mean = mean * (1.0 / count)
                spread = None
                for ref, own_mean in zip(sums, means):
                    off = own_mean - mean
                    part = ref[1, n, here] + J * (off * off)
                    spread = part if spread is None else spread + part
                scale = lax.rsqrt(spread * (1.0 / (J * count)) + 0.0001)
                for j in range(J):
                    scaled[j, n, here] = (u[j, n, here] - mean) * scale
                return carry

            lax.fori_loop(0, kc // ROWS, tile, 0)
            copies.append(pltpu.make_async_copy(scaled.at[:, n], anomaly_out.at[:, i, pl.ds(k0, kc)], sems.at[nl + n]))
            copies[-1].start()
        for copy in copies:
            copy.wait()

    full = jax.ShapeDtypeStruct(shape, F32)
    ins = [new, own] + list(others)
    aliases = {len(ins): 0, len(ins) + 1: 1} if buffers else {}
    return call(
        body,
        ins + list(buffers),
        [VMEM] * len(ins) + [HBM] * len(buffers),
        [full, full],
        [HBM, HBM],
        f"finish_{k0}_{'_'.join(map(str, layers))}",
        [pltpu.VMEM((J, nl, kc, L), F32), pltpu.SemaphoreType.DMA((2 * nl,))],
        aliases,
        flops=10 * J * nl * kc * L,
    )


def other_rows(own):
    count = lax.axis_size("rows")
    return [lax.ppermute(own, "rows", [(i, (i + shift) % count) for i in range(count)]) for shift in range(1, count)]


def spans_of(extent):
    tiles = extent // ROWS
    cuts = [tiles * n // CHUNKS * ROWS for n in range(CHUNKS + 1)]
    return [(a, b - a) for a, b in zip(cuts, cuts[1:])]


def on_device(field_values, conductance, source):
    shape = J, I, K, L = field_values.shape
    spans = spans_of(K)
    chunks = range(len(spans))
    z_out, y_out, x_out = first_faces(field_values, spans)
    z_in = [exchange(z_out[q], "cols", ("up", "down")) for q in chunks]
    y_in = [exchange(y_out[q], "rows") for q in chunks]
    x_in = exchange(x_out, "slabs")
    fields, cond, src = load([field_values, conductance, source], spans)
    for _ in range(STEPS - 1):
        newer, z_next, y_next = [], [], []
        for q in chunks:
            new, z, y, x_out = step(
                q, fields, cond[q], src[q], z_in[q], y_in[q], x_in, range(I), False, newer[0] if newer else None
            )
            newer.append(new)
            z_next.append(exchange(z, "cols", ("up", "down")))
            y_next.append(exchange(y, "rows"))
        x_in = exchange(x_out, "slabs")
        fields, z_in, y_in = newer, z_next, y_next

    buffers = []
    inner, outer = list(range(1, I - 1)), [0, I - 1]
    parts = [(inner, q) for q in chunks] + [(outer, q) for q in chunks]
    for layers, q in parts:
        faces = z_in[q] if layers is outer else None
        new, own = step(q, fields, cond[q], src[q], faces, y_in[q], x_in, layers, True, None)
        buffers = finish(new, own, other_rows(own), layers, spans[q], buffers, shape)
    return tuple(buffers)


def solution(mesh):
    spec = P(("trial", "rows"), "cols", "slabs", None)
    return jax.shard_map(
        on_device, mesh=mesh, in_specs=(spec, spec, spec), out_specs=(spec, spec), check_vma=False
    )
```

```python
import jax
import jax.numpy as jnp
from jax import lax
from jax.experimental import pallas as pl
from jax.experimental.pallas import tpu as pltpu
from jax.sharding import PartitionSpec as P

STEPS = 4
CHUNKS = 2
ROWS = 8
HBM = pl.BlockSpec(memory_space=pltpu.HBM)
VMEM = pl.BlockSpec(memory_space=pltpu.VMEM)
F32 = jnp.float32


def vmem(*shape):
    return pltpu.VMEM(shape, F32)


def call(body, ins, in_specs, outs, out_specs, name, scratch=(), aliases=None, flops=0):
    return pl.pallas_call(
        body,
        in_specs=in_specs,
        out_shape=outs,
        out_specs=out_specs,
        scratch_shapes=scratch,
        input_output_aliases=aliases or {},
        compiler_params=pltpu.CompilerParams(vmem_limit_bytes=12 * 2**20),
        cost_estimate=pl.CostEstimate(flops=flops, bytes_accessed=0, transcendentals=0) if flops else None,
        name=name,
    )(*ins)


def ports_of(axis):
    return (0,) if lax.axis_size(axis) == 2 else (0, 1)


def exchange(buffers, axis):
    count = lax.axis_size(axis)
    received = []
    for port, buffer in zip(ports_of(axis), buffers):
        perm = []
        for i in range(port, count - 1, 2):
            perm += [(i, i + 1), (i + 1, i)]
        received.append(lax.ppermute(buffer, axis, perm))
    return received


def is_upper(axis, port):
    odd = lax.axis_index(axis) % 2
    return odd if port == 0 else 1 - odd


def sent_index(axis, port, extent):
    return (1 - is_upper(axis, port)) * (extent - 1)


def halo_readers(axis, refs):
    upper = is_upper(axis, 0)
    if len(refs) == 1:
        has_lower = upper.astype(F32)
        has_upper = (1 - upper).astype(F32)
        return (lambda where: refs[0][where] * has_lower), (lambda where: refs[0][where] * has_upper)
    return (
        lambda where: jnp.where(upper == 1, refs[0][where], refs[1][where]),
        lambda where: jnp.where(upper == 1, refs[1][where], refs[0][where]),
    )


def run_copies(copies):
    for copy in copies:
        copy.start()
    for copy in copies:
        copy.wait()


def first_faces(field, spans):
    J, I, K, L = field.shape
    z_ports, y_ports, x_ports = ports_of("cols"), ports_of("rows"), ports_of("slabs")

    def body(u, *refs):
        outs, sems = list(refs[:-1]), refs[-1]
        pairs = []
        for k0, kc in spans:
            for port in z_ports:
                pairs.append((u.at[:, sent_index("cols", port, I), pl.ds(k0, kc)], outs.pop(0)))
            for port in y_ports:
                pairs.append((u.at[sent_index("rows", port, J), :, pl.ds(k0, kc)], outs.pop(0)))
        for port in x_ports:
            pairs.append((u.at[:, :, sent_index("slabs", port, K)], outs.pop(0)))
        run_copies([pltpu.make_async_copy(src, dst, sems.at[n]) for n, (src, dst) in enumerate(pairs)])

    shapes = []
    for _, kc in spans:
        shapes += [vmem(J, kc, L)] * len(z_ports) + [vmem(I, kc, L)] * len(y_ports)
    shapes += [vmem(J, I, L)] * len(x_ports)
    outs = list(
        call(body, [field], [HBM], shapes, [VMEM] * len(shapes), "first_faces", [pltpu.SemaphoreType.DMA((len(shapes),))])
    )
    z, y = [], []
    for _ in spans:
        z.append([outs.pop(0) for _ in z_ports])
        y.append([outs.pop(0) for _ in y_ports])
    return z, y, outs


def step(q, spans, fields, cond, src, z_in, y_in, x_in, layers, last, newer):
    J, I, _, L = cond.shape
    k0, kc = spans[q]
    z_ports, y_ports, x_ports = ports_of("cols"), ports_of("rows"), ports_of("slabs")
    send_x = not last and q == len(spans) - 1
    below = fields[q - 1] if q > 0 else None
    above = fields[q + 1] if q + 1 < len(spans) else None
    ins = [fields[q][0], cond, src] + [a[0] for a in (below, above) if a is not None] + list(z_in) + list(y_in) + list(x_in)
    if send_x:
        ins.append(newer)
    nl = len(layers)
    base = k0 - fields[q][1]

    def body(*refs):
        refs = list(refs)
        u, c, s = refs.pop(0), refs.pop(0), refs.pop(0)
        lower_u = refs.pop(0) if below is not None else None
        upper_u = refs.pop(0) if above is not None else None
        z = [refs.pop(0) for _ in z_in]
        y = [refs.pop(0) for _ in y_in]
        x = [refs.pop(0) for _ in x_in]
        first_u = refs.pop(0) if send_x else None
        out = refs.pop(0)
        if z:
            z_lo, z_hi = halo_readers("cols", z)
        y_lo, y_hi = halo_readers("rows", y)
        x_lo, x_hi = halo_readers("slabs", x)
        sublane = lax.broadcasted_iota(jnp.int32, (ROWS, L), 0)

        def tile(k, at_low, at_high):
            here = pl.ds(k, ROWS)
            known = {}

            def cells(j, i):
                if (j, i) not in known:
                    if j < 0:
                        known[j, i] = y_lo((i, here))
                    elif j >= J:
                        known[j, i] = y_hi((i, here))
                    elif i < 0:
                        known[j, i] = z_lo((j, here))
                    elif i >= I:
                        known[j, i] = z_hi((j, here))
                    else:
                        known[j, i] = u[j, i, pl.ds(k + base, ROWS)]
                return known[j, i]

            def edge_row(ref, j, i, row):
                return jnp.broadcast_to(ref[j, i, pl.ds(row, 1)], (ROWS, L))

            def k_lower(j, i):
                if not at_low:
                    return u[j, i, pl.ds(k + base - 1, ROWS)]
                if lower_u is not None:
                    edge = edge_row(lower_u, j, i, k0 - 1 - below[1])
                else:
                    edge = jnp.broadcast_to(x_lo((j, pl.ds(i, 1))), (ROWS, L))
                return jnp.where(sublane == 0, edge, pltpu.roll(cells(j, i), 1, 0))

            def k_upper(j, i):
                if not at_high:
                    return u[j, i, pl.ds(k + base + 1, ROWS)]
                if upper_u is not None:
                    edge = edge_row(upper_u, j, i, k0 + kc - above[1])
                else:
                    edge = jnp.broadcast_to(x_hi((j, pl.ds(i, 1))), (ROWS, L))
                return jnp.where(sublane == ROWS - 1, edge, pltpu.roll(cells(j, i), ROWS - 1, 0))

            totals = [None] * nl
            for j in range(J):
                for n, i in enumerate(layers):
                    middle = cells(j, i)
                    spread = (
                        (cells(j - 1, i) + cells(j + 1, i))
                        + (cells(j, i - 1) + cells(j, i + 1))
                        + (k_lower(j, i) + k_upper(j, i))
                        - 6.0 * middle
                    )
                    new = middle + c[j, i, pl.ds(k + k0, ROWS)] * spread + s[j, i, pl.ds(k + k0, ROWS)]
                    out[j, n, here] = new
                    if last:
                        totals[n] = new if j == 0 else totals[n] + new
                    elif i == 0:
                        lowest = new
                    elif i == I - 1:
                        highest = new
                if not last:
                    for ref, port in zip(z_out, z_ports):
                        ref[j, here] = jnp.where(is_upper("cols", port) == 1, lowest, highest)
                for i in list(known):
                    if i[0] < j:
                        del known[i]
            if last:
                for n in range(nl):
                    mean = totals[n] * (1.0 / J)
                    spread = None
                    for j in range(J):
                        off = out[j, n, here] - mean
                        spread = off * off if j == 0 else spread + off * off
                    stats[0, n, here] = mean
                    stats[1, n, here] = spread

        if last:
            stats = refs.pop(0)
        else:
            z_out = [refs.pop(0) for _ in z_ports]
            y_out = [refs.pop(0) for _ in y_ports]
            x_out = [refs.pop(0) for _ in x_ports] if send_x else []

        tiles = kc // ROWS
        tile(0, True, tiles == 1)
        if tiles > 2:

            def inner(t, carry):
                tile(pl.multiple_of(t * ROWS, ROWS), False, False)
                return carry

            lax.fori_loop(1, tiles - 1, inner, 0)
        if tiles > 1:
            tile(kc - ROWS, False, True)
        if not last:
            for ref, port in zip(y_out, y_ports):
                ref[...] = out[sent_index("rows", port, J)]
            for ref, port in zip(x_out, x_ports):
                for j in range(J):
                    head = first_u[j, :, 0, :]
                    tail = out[j, :, kc - 1, :]
                    upper = is_upper("slabs", port).astype(F32)
                    ref[j] = head * upper + tail * (1.0 - upper)

    shapes = [vmem(J, nl, kc, L)]
    if last:
        shapes.append(vmem(2, nl, kc, L))
    else:
        shapes += [vmem(J, kc, L)] * len(z_ports) + [vmem(I, kc, L)] * len(y_ports)
        if send_x:
            shapes += [vmem(J, I, L)] * len(x_ports)
    outs = list(
        call(
            body,
            ins,
            [VMEM] * len(ins),
            shapes,
            [VMEM] * len(shapes),
            f"step_{'last' if last else 'mid'}_{q}_{'_'.join(map(str, layers))}",
            flops=10 * J * nl * kc * L,
        )
    )
    new = outs.pop(0)
    if last:
        return new, outs[0]
    z = [outs.pop(0) for _ in z_ports]
    y = [outs.pop(0) for _ in y_ports]
    return new, z, y, outs


def finish(new, own, others, layers, span, buffers, shape):
    J, I, K, L = shape
    k0, kc = span
    nl = len(layers)
    count = len(others) + 1

    def body(*refs):
        refs = list(refs)
        u = refs.pop(0)
        sums = [refs.pop(0) for _ in range(count)]
        if buffers:
            refs.pop(0), refs.pop(0)
        anomaly_out, field_out, scaled, sems = refs
        copies = []
        for n, i in enumerate(layers):
            copies.append(pltpu.make_async_copy(u.at[:, n], field_out.at[:, i, pl.ds(k0, kc)], sems.at[n]))
            copies[-1].start()

        for n, i in enumerate(layers):

            def tile(t, carry):
                here = pl.ds(pl.multiple_of(t * ROWS, ROWS), ROWS)
                means = [ref[0, n, here] for ref in sums]
                mean = means[0]
                for other in means[1:]:
                    mean = mean + other
                mean = mean * (1.0 / count)
                spread = None
                for ref, own_mean in zip(sums, means):
                    off = own_mean - mean
                    part = ref[1, n, here] + J * (off * off)
                    spread = part if spread is None else spread + part
                scale = lax.rsqrt(spread * (1.0 / (J * count)) + 0.0001)
                for j in range(J):
                    scaled[j, n, here] = (u[j, n, here] - mean) * scale
                return carry

            lax.fori_loop(0, kc // ROWS, tile, 0)
            copies.append(pltpu.make_async_copy(scaled.at[:, n], anomaly_out.at[:, i, pl.ds(k0, kc)], sems.at[nl + n]))
            copies[-1].start()
        for copy in copies:
            copy.wait()

    full = jax.ShapeDtypeStruct(shape, F32)
    ins = [new, own] + list(others)
    aliases = {len(ins): 0, len(ins) + 1: 1} if buffers else {}
    return call(
        body,
        ins + list(buffers),
        [VMEM] * len(ins) + [HBM] * len(buffers),
        [full, full],
        [HBM, HBM],
        f"finish_{k0}_{'_'.join(map(str, layers))}",
        [pltpu.VMEM((J, nl, kc, L), F32), pltpu.SemaphoreType.DMA((2 * nl,))],
        aliases,
        flops=10 * J * nl * kc * L,
    )


def other_rows(own):
    count = lax.axis_size("rows")
    return [lax.ppermute(own, "rows", [(i, (i + shift) % count) for i in range(count)]) for shift in range(1, count)]


def spans_of(extent):
    tiles = extent // ROWS
    cuts = [tiles * n // CHUNKS * ROWS for n in range(CHUNKS + 1)]
    return [(a, b - a) for a, b in zip(cuts, cuts[1:])]


def on_device(field_values, conductance, source):
    shape = J, I, K, L = field_values.shape
    spans = spans_of(K)
    chunks = range(len(spans))
    z_out, y_out, x_out = first_faces(field_values, spans)
    z_in = [exchange(z_out[q], "cols") for q in chunks]
    y_in = [exchange(y_out[q], "rows") for q in chunks]
    x_in = exchange(x_out, "slabs")
    fields = [(field_values, 0) for _ in chunks]
    for _ in range(STEPS - 1):
        newer, z_next, y_next = [], [], []
        for q in chunks:
            new, z, y, x_out = step(
                q, spans, fields, conductance, source, z_in[q], y_in[q], x_in, range(I), False, newer[0][0] if newer else None
            )
            newer.append((new, spans[q][0]))
            z_next.append(exchange(z, "cols"))
            y_next.append(exchange(y, "rows"))
        x_in = exchange(x_out, "slabs")
        fields, z_in, y_in = newer, z_next, y_next

    buffers = []
    inner, outer = list(range(1, I - 1)), [0, I - 1]
    for layers in (inner, outer):
        for q in chunks:
            if layers:
                faces = z_in[q] if layers is outer else []
                new, own = step(q, spans, fields, conductance, source, faces, y_in[q], x_in, layers, True, None)
                buffers = finish(new, own, other_rows(own), layers, spans[q], buffers, shape)
    return tuple(buffers)


def solution(mesh):
    spec = P(("trial", "rows"), "cols", "slabs", None)
    return jax.shard_map(
        on_device, mesh=mesh, in_specs=(spec, spec, spec), out_specs=(spec, spec), check_vma=False
    )
```

```python
import jax
import jax.numpy as jnp
from jax import lax
from jax.experimental import pallas as pl
from jax.experimental.pallas import tpu as pltpu
from jax.sharding import PartitionSpec as P


STEPS = 4
CHUNKS = (9, 7)
LAST_CUT = (5, 2)
ROWS = 8
HBM = pl.BlockSpec(memory_space=pltpu.HBM)
VMEM = pl.BlockSpec(memory_space=pltpu.VMEM)
F32 = jnp.float32


def vmem(*shape):
    return pltpu.VMEM(shape, F32)


def call(body, ins, in_specs, outs, out_specs, scratch=(), aliases=None, flops=0):
    return pl.pallas_call(
        body,
        in_specs=in_specs,
        out_shape=outs,
        out_specs=out_specs,
        scratch_shapes=scratch,
        input_output_aliases=aliases or {},
        compiler_params=pltpu.CompilerParams(vmem_limit_bytes=12 * 2**20),
        cost_estimate=pl.CostEstimate(flops=flops, bytes_accessed=0, transcendentals=0) if flops else None,
    )(*ins)


def ports_of(axis):
    return (0,) if lax.axis_size(axis) == 2 else (0, 1)


def exchange(buffers, axis):
    count = lax.axis_size(axis)
    received = []
    for port, buffer in zip(ports_of(axis), buffers):
        perm = []
        for i in range(port, count - 1, 2):
            perm += [(i, i + 1), (i + 1, i)]
        received.append(lax.ppermute(buffer, axis, perm))
    return received


def is_upper(axis, port):
    odd = lax.axis_index(axis) % 2
    return odd if port == 0 else 1 - odd


def sent_index(axis, port, extent):
    return (1 - is_upper(axis, port)) * (extent - 1)


def halo_readers(axis, refs):
    upper = is_upper(axis, 0)
    if len(refs) == 1:
        has_lower = upper.astype(F32)
        has_upper = (1 - upper).astype(F32)
        return (lambda where: refs[0][where] * has_lower), (lambda where: refs[0][where] * has_upper)
    return (
        lambda where: jnp.where(upper == 1, refs[0][where], refs[1][where]),
        lambda where: jnp.where(upper == 1, refs[1][where], refs[0][where]),
    )


def run_copies(copies):
    for copy in copies:
        copy.start()
    for copy in copies:
        copy.wait()


def write_copies(cells, out, layers, first, rows, sems):
    return [
        pltpu.make_async_copy(cells.at[:, n], out.at[:, i, pl.ds(first, rows)], sems.at[n]) for n, i in enumerate(layers)
    ]


def cut_faces(field, z_spans, y_spans, with_x):
    J, I, K, L = field.shape
    z_ports, y_ports, x_ports = ports_of("cols"), ports_of("rows"), ports_of("slabs") if with_x else ()
    shapes = [vmem(J, kc, L) for _, kc in z_spans for _ in z_ports]
    shapes += [vmem(I, kc, L) for _, kc in y_spans for _ in y_ports]
    shapes += [vmem(J, I, L) for _ in x_ports]

    def body(u, *refs):
        sources = [u.at[:, sent_index("cols", port, I), pl.ds(k0, kc)] for k0, kc in z_spans for port in z_ports]
        sources += [u.at[sent_index("rows", port, J), :, pl.ds(k0, kc)] for k0, kc in y_spans for port in y_ports]
        sources += [u.at[:, :, sent_index("slabs", port, K)] for port in x_ports]
        run_copies([pltpu.make_async_copy(src, refs[n], refs[-1].at[n]) for n, src in enumerate(sources)])

    field = pltpu.with_memory_space_constraint(field, pltpu.HBM)
    outs = list(call(body, [field], [HBM], shapes, [VMEM] * len(shapes), [pltpu.SemaphoreType.DMA((len(shapes),))]))
    z = [[outs.pop(0) for _ in z_ports] for _ in z_spans]
    y = [[outs.pop(0) for _ in y_ports] for _ in y_spans]
    return z, y, outs


def stage(arrays):
    def body(*refs):
        n = len(arrays)
        run_copies([pltpu.make_async_copy(refs[m], refs[n + m], refs[-1].at[m]) for m in range(n)])

    held = [pltpu.with_memory_space_constraint(array, pltpu.HBM) for array in arrays]
    shapes = [vmem(*array.shape) for array in arrays]
    return call(body, held, [HBM] * len(held), shapes, [VMEM] * len(held), [pltpu.SemaphoreType.DMA((len(held),))])


def step(pieces, fields, cond, src, y_in, x_in, layers, z_spans, x_head, last, write=None):
    J, I, K, L = cond.shape
    nl = len(layers)
    z_ports, y_ports, x_ports = ports_of("cols"), ports_of("rows"), ports_of("slabs")
    first = pieces[0][1]
    rows = sum(piece[2] for piece in pieces)
    ins, slots = [], {}

    def add(array):
        if id(array) not in slots:
            slots[id(array)] = len(ins)
            ins.append(array)
        return slots[id(array)]

    cond_at, src_at = add(cond), add(src)
    near = {q + d for q, *_ in pieces for d in (-1, 0, 1)} & set(range(len(fields)))
    field_at = {q: add(fields[q][0]) for q in sorted(near)}
    z_at = [[add(array) for array in piece[3]] for piece in pieces]
    y_at = {q: [add(array) for array in y_in[q][0]] for q, *_ in pieces}
    x_at = [add(array) for array in x_in]
    head_at = add(x_head) if x_head is not None else None
    if write is not None:
        done, done_layers, (done_first, done_rows), buffer = write
        done_at = add(done)
        buffers = [] if buffer is None else [buffer]

    def body(*refs):
        if write is not None:
            copies = write_copies(refs[done_at], refs[-2], done_layers, done_first, done_rows, refs[-1])
            for copy in copies:
                copy.start()
            compute(refs[: len(ins)] + refs[len(ins) + len(buffers) : -2])
            for copy in copies:
                copy.wait()
        else:
            compute(refs)

    def compute(refs):
        outs = list(refs[len(ins) :])
        c, s = refs[cond_at], refs[src_at]
        out = outs.pop(0)
        if last:
            stats = outs.pop(0)
        else:
            z_out = [[outs.pop(0) for _ in z_ports] for _ in z_spans]
            y_out = [outs.pop(0) for _ in y_ports]
            x_out = [outs.pop(0) for _ in x_ports] if x_head is not None else []
        x_lo, x_hi = halo_readers("slabs", [refs[n] for n in x_at])
        sublane = lax.broadcasted_iota(jnp.int32, (ROWS, L), 0)

        def tile(k, q, z, z_first, z_to, z_to_first, at_low, at_high):
            u, base = refs[field_at[q]], fields[q][1]
            y_lo, y_hi = halo_readers("rows", [refs[n] for n in y_at[q]])
            if z:
                z_lo, z_hi = halo_readers("cols", z)
            in_y = pl.ds(k - y_in[q][1], ROWS)
            in_z = pl.ds(k - z_first, ROWS)
            here = pl.ds(k - first, ROWS)
            there = pl.ds(k, ROWS)
            known = {}

            def cells(j, i):
                if (j, i) not in known:
                    if j < 0:
                        known[j, i] = y_lo((i, in_y))
                    elif j >= J:
                        known[j, i] = y_hi((i, in_y))
                    elif i < 0:
                        known[j, i] = z_lo((j, in_z))
                    elif i >= I:
                        known[j, i] = z_hi((j, in_z))
                    else:
                        known[j, i] = u[j, i, pl.ds(k - base, ROWS)]
                return known[j, i]

            def edge_row(near_q, j, i, row):
                array, start = refs[field_at[near_q]], fields[near_q][1]
                return jnp.broadcast_to(array[j, i, pl.ds(row - start, 1)], (ROWS, L))

            def k_lower(j, i):
                if not at_low:
                    return u[j, i, pl.ds(k - base - 1, ROWS)]
                if q > 0:
                    edge = edge_row(q - 1, j, i, k - 1)
                else:
                    edge = jnp.broadcast_to(x_lo((j, pl.ds(i, 1))), (ROWS, L))
                return jnp.where(sublane == 0, edge, pltpu.roll(cells(j, i), 1, 0))

            def k_upper(j, i):
                if not at_high:
                    return u[j, i, pl.ds(k - base + 1, ROWS)]
                if q + 1 < len(fields):
                    edge = edge_row(q + 1, j, i, k + ROWS)
                else:
                    edge = jnp.broadcast_to(x_hi((j, pl.ds(i, 1))), (ROWS, L))
                return jnp.where(sublane == ROWS - 1, edge, pltpu.roll(cells(j, i), ROWS - 1, 0))

            totals = [None] * nl
            for j in range(J):
                for n, i in enumerate(layers):
                    middle = cells(j, i)
                    spread = (
                        (cells(j - 1, i) + cells(j + 1, i))
                        + (cells(j, i - 1) + cells(j, i + 1))
                        + (k_lower(j, i) + k_upper(j, i))
                        - 6.0 * middle
                    )
                    new = middle + c[j, i, there] * spread + s[j, i, there]
                    out[j, n, here] = new
                    if last:
                        totals[n] = new if j == 0 else totals[n] + new
                    if i == 0:
                        lowest = new
                    if i == I - 1:
                        highest = new
                if not last:
                    for ref, port in zip(z_to, z_ports):
                        ref[j, pl.ds(k - z_to_first, ROWS)] = jnp.where(is_upper("cols", port) == 1, lowest, highest)
                for at in list(known):
                    if at[0] < j:
                        del known[at]
            if last:
                for n in range(nl):
                    mean = totals[n] * (1.0 / J)
                    spread = None
                    for j in range(J):
                        off = out[j, n, here] - mean
                        spread = off * off if j == 0 else spread + off * off
                    stats[0, n, here] = mean
                    stats[1, n, here] = spread

        for (q, k0, kc, _), z_refs in zip(pieces, z_at):
            z = [refs[n] for n in z_refs]
            array_low, array_high = fields[q][1], fields[q][1] + fields[q][0].shape[2]
            targets = [(0, K, None)] if last else [(*span, n) for n, span in enumerate(z_spans)]
            for t0, tc, n in targets:
                low, high = max(k0, t0), min(k0 + kc, t0 + tc)
                if low >= high:
                    continue
                z_to = z_out[n] if n is not None else []
                same = (q, z, k0, z_to, t0)
                begin, end = low, high
                if low == array_low:
                    tile(low, *same, True, low + ROWS == array_high)
                    begin += ROWS
                if high == array_high and begin < high:
                    tile(high - ROWS, *same, False, True)
                    end -= ROWS
                if begin < end:

                    def inner(t, carry, same=same):
                        tile(pl.multiple_of(t * ROWS, ROWS), *same, False, False)
                        return carry

                    lax.fori_loop(begin // ROWS, end // ROWS, inner, 0)
        if not last:
            for ref, port in zip(y_out, y_ports):
                ref[...] = out[sent_index("rows", port, J)]
            for ref, port in zip(x_out, x_ports):
                for j in range(J):
                    head = refs[head_at][j, :, 0, :]
                    tail = out[j, :, rows - 1, :]
                    upper = is_upper("slabs", port).astype(F32)
                    ref[j] = head * upper + tail * (1.0 - upper)

    shapes = [vmem(J, nl, rows, L)]
    if last:
        shapes.append(vmem(2, nl, rows, L))
    else:
        for _, tc in z_spans:
            shapes += [vmem(J, tc, L)] * len(z_ports)
        shapes += [vmem(I, rows, L)] * len(y_ports)
        if x_head is not None:
            shapes += [vmem(J, I, L)] * len(x_ports)
    all_ins, in_specs, out_specs, scratch, aliases = ins, [VMEM] * len(ins), [VMEM] * len(shapes), [], None
    if write is not None:
        all_ins, in_specs = ins + buffers, in_specs + [HBM] * len(buffers)
        aliases = {len(ins): len(shapes)} if buffers else None
        shapes, out_specs = shapes + [jax.ShapeDtypeStruct(cond.shape, F32)], out_specs + [HBM]
        scratch = [pltpu.SemaphoreType.DMA((len(done_layers),))]
    outs = list(call(body, all_ins, in_specs, shapes, out_specs, scratch, aliases, flops=10 * J * nl * rows * L))
    new = outs.pop(0)
    if last:
        return new, outs[0], outs[1] if write is not None else None
    z = [[outs.pop(0) for _ in z_ports] for _ in z_spans]
    y = [outs.pop(0) for _ in y_ports]
    return new, z, y, outs


def finish(new, own, others, layers, span, anomaly, field, shape):
    J, _, _, L = shape
    k0, kc = span
    nl = len(layers)
    count = len(others) + 1
    buffers = [buffer for buffer in (anomaly, field) if buffer is not None]
    outs_count = 1 if field is None else 2

    def body(*refs):
        u, sums = refs[0], refs[1 : 1 + count]
        outs = refs[1 + count + len(buffers) : 1 + count + len(buffers) + outs_count]
        scaled, sems = refs[-2:]
        copies = []
        if field is not None:
            copies += write_copies(u, outs[1], layers, k0, kc, sems.at[1])
            for copy in copies:
                copy.start()
        results = write_copies(scaled, outs[0], layers, k0, kc, sems.at[0])
        for n in range(nl):

            def tile(t, carry, n=n):
                here = pl.ds(pl.multiple_of(t * ROWS, ROWS), ROWS)
                means = [ref[0, n, here] for ref in sums]
                mean = means[0]
                for other in means[1:]:
                    mean = mean + other
                mean = mean * (1.0 / count)
                spread = None
                for ref, own_mean in zip(sums, means):
                    off = own_mean - mean
                    part = ref[1, n, here] + J * (off * off)
                    spread = part if spread is None else spread + part
                scale = lax.rsqrt(spread * (1.0 / (J * count)) + 0.0001)
                for j in range(J):
                    scaled[j, n, here] = (u[j, n, here] - mean) * scale
                return carry

            lax.fori_loop(0, kc // ROWS, tile, 0)
            results[n].start()
        for copy in copies + results:
            copy.wait()

    ins = [new, own] + list(others)
    aliases = {len(ins) + n: (n if anomaly is not None else 1) for n in range(len(buffers))}
    return call(
        body,
        ins + buffers,
        [VMEM] * len(ins) + [HBM] * len(buffers),
        [jax.ShapeDtypeStruct(shape, F32)] * outs_count,
        [HBM] * outs_count,
        [pltpu.VMEM((J, nl, kc, L), F32), pltpu.SemaphoreType.DMA((2, nl))],
        aliases,
        flops=10 * J * nl * kc * L,
    )


def other_rows(own):
    count = lax.axis_size("rows")
    return [lax.ppermute(own, "rows", [(i, (i + shift) % count) for i in range(count)]) for shift in range(1, count)]


def spans_of(start, extent, weights):
    tiles, total, cuts = extent // ROWS, sum(weights), [0]
    for n in range(1, len(weights) + 1):
        cuts.append(round(tiles * sum(weights[:n]) / total))
    return [(start + a * ROWS, (b - a) * ROWS) for a, b in zip(cuts, cuts[1:]) if b > a]


def on_device(field_values, conductance, source):
    shape = J, I, K, L = field_values.shape
    spans = spans_of(0, K, CHUNKS)
    chunks = range(len(spans))

    def trade(z, y):
        z_got = []
        for faces in z:
            z_got.append(exchange(faces, "cols"))
        return z_got, exchange(y, "rows")

    z_out = cut_faces(field_values, spans[:1], [], False)[0]
    z_rest, y_out, x_out = cut_faces(field_values, spans[1:], spans, True)
    z_out += z_rest
    z_in, y_in = [], []
    for q in chunks:
        z_got, y_got = trade([z_out[q]], y_out[q])
        z_in.append([(*spans[q], z_got[0])])
        y_in.append((y_got, spans[q][0]))
    x_in = exchange(x_out, "slabs")
    staged, conductance, source = stage([field_values, conductance, source])
    fields = [(staged, 0) for _ in chunks]
    for step_no in range(1, STEPS):
        newer, z_next, y_next = [], [], []
        for q in chunks:
            is_end = q == len(spans) - 1
            z_spans = spans_of(*spans[q], LAST_CUT) if is_end and step_no == STEPS - 1 else [spans[q]]
            pieces = [(q, k0, kc, faces) for k0, kc, faces in z_in[q]]
            new, z, y, x_out = step(
                pieces,
                fields,
                conductance,
                source,
                y_in,
                x_in,
                range(I),
                z_spans,
                (newer + [(None, 0)])[0][0] if is_end else None,
                False,
            )
            newer.append((new, spans[q][0]))
            z_got, y_got = trade(z, y)
            z_next.append([(*span, faces) for span, faces in zip(z_spans, z_got)])
            y_next.append((y_got, spans[q][0]))
        x_in = exchange(x_out, "slabs")
        fields, z_in, y_in = newer, z_next, y_next

    inner, outer = list(range(1, I - 1)), [0, I - 1]
    jobs = []
    if inner:
        jobs.append((inner, [(q, *spans[q], []) for q in chunks]))
    for q in chunks:
        for k0, kc, faces in z_in[q]:
            jobs.append((outer, [(q, k0, kc, faces)]))
    anomaly, field, write, sums = None, None, None, []
    for n, (layers, pieces) in enumerate(jobs):
        new, own, wrote = step(pieces, fields, conductance, source, y_in, x_in, layers, [], None, True, write)
        field = field if wrote is None else wrote
        others = other_rows(own)
        span = (pieces[0][1], sum(piece[2] for piece in pieces))
        write = (new, layers, span, field) if n < len(jobs) - 2 else None
        sums.append((new, own, others, layers, span))
    for n, job in enumerate(sums):
        to_field = field if n >= len(sums) - 2 else None
        done = finish(*job, anomaly, to_field, shape)
        anomaly = done[0]
        field = done[1] if to_field is not None else field
    return anomaly, field


def solution(mesh):
    spec = P(("trial", "rows"), "cols", "slabs", None)

    return jax.shard_map(on_device, mesh=mesh, in_specs=(spec, spec, spec), out_specs=(spec, spec), check_vma=False)
```

```python
import jax
import jax.numpy as jnp
from jax import lax
from jax.experimental import pallas as pl
from jax.experimental.pallas import tpu as pltpu
from jax.sharding import PartitionSpec as P


STEPS = 4
CHUNKS = (9, 7)
LAST_CUT = (5, 2)
ROWS = 8
HBM = pl.BlockSpec(memory_space=pltpu.HBM)
VMEM = pl.BlockSpec(memory_space=pltpu.VMEM)
F32 = jnp.float32


def vmem(*shape):
    return pltpu.VMEM(shape, F32)


def call(body, ins, in_specs, outs, out_specs, scratch=(), aliases=None, flops=0):
    return pl.pallas_call(
        body,
        in_specs=in_specs,
        out_shape=outs,
        out_specs=out_specs,
        scratch_shapes=scratch,
        input_output_aliases=aliases or {},
        compiler_params=pltpu.CompilerParams(vmem_limit_bytes=12 * 2**20),
        cost_estimate=pl.CostEstimate(flops=flops, bytes_accessed=0, transcendentals=0) if flops else None,
    )(*ins)


def ports_of(axis):
    return (0,) if lax.axis_size(axis) == 2 else (0, 1)


def exchange(buffers, axis):
    count, trials = lax.axis_size(axis), lax.axis_size("trial")
    received = []
    for port, buffer in zip(ports_of(axis), buffers):
        pairs, alone = [], set(range(count))
        for i in range(port, count - 1, 2):
            pairs += [(i * trials + t, (i + 1) * trials + t) for t in range(trials)]
            alone -= {i, i + 1}
        pairs += [(i * trials + t, i * trials + t + 1) for i in sorted(alone) for t in range(0, trials - 1, 2)]
        received.append(lax.ppermute(buffer, (axis, "trial"), pairs + [(b, a) for a, b in pairs]))
    return received


def is_upper(axis, port):
    odd = lax.axis_index(axis) % 2
    return odd if port == 0 else 1 - odd


def sent_index(axis, port, extent):
    return (1 - is_upper(axis, port)) * (extent - 1)


def halo_readers(axis, refs):
    at, upper = lax.axis_index(axis), is_upper(axis, 0)
    has_lower = (at > 0).astype(F32)
    has_upper = (at < lax.axis_size(axis) - 1).astype(F32)
    if len(refs) == 1:
        return (lambda where: refs[0][where] * has_lower), (lambda where: refs[0][where] * has_upper)
    return (
        lambda where: jnp.where(upper == 1, refs[0][where], refs[1][where]) * has_lower,
        lambda where: jnp.where(upper == 1, refs[1][where], refs[0][where]) * has_upper,
    )


def run_copies(copies):
    for copy in copies:
        copy.start()
    for copy in copies:
        copy.wait()


def write_copies(cells, out, layers, first, rows, sems):
    return [
        pltpu.make_async_copy(cells.at[:, n], out.at[:, i, pl.ds(first, rows)], sems.at[n]) for n, i in enumerate(layers)
    ]


def cut_faces(field, z_spans, y_spans, with_x):
    J, I, K, L = field.shape
    z_ports, y_ports, x_ports = ports_of("cols"), ports_of("rows"), ports_of("slabs") if with_x else ()
    shapes = [vmem(J, kc, L) for _, kc in z_spans for _ in z_ports]
    shapes += [vmem(I, kc, L) for _, kc in y_spans for _ in y_ports]
    shapes += [vmem(J, I, L) for _ in x_ports]

    def body(u, *refs):
        sources = [u.at[:, sent_index("cols", port, I), pl.ds(k0, kc)] for k0, kc in z_spans for port in z_ports]
        sources += [u.at[sent_index("rows", port, J), :, pl.ds(k0, kc)] for k0, kc in y_spans for port in y_ports]
        sources += [u.at[:, :, sent_index("slabs", port, K)] for port in x_ports]
        run_copies([pltpu.make_async_copy(src, refs[n], refs[-1].at[n]) for n, src in enumerate(sources)])

    field = pltpu.with_memory_space_constraint(field, pltpu.HBM)
    outs = list(call(body, [field], [HBM], shapes, [VMEM] * len(shapes), [pltpu.SemaphoreType.DMA((len(shapes),))]))
    z = [[outs.pop(0) for _ in z_ports] for _ in z_spans]
    y = [[outs.pop(0) for _ in y_ports] for _ in y_spans]
    return z, y, outs


def stage(arrays):
    def body(*refs):
        n = len(arrays)
        run_copies([pltpu.make_async_copy(refs[m], refs[n + m], refs[-1].at[m]) for m in range(n)])

    held = [pltpu.with_memory_space_constraint(array, pltpu.HBM) for array in arrays]
    shapes = [vmem(*array.shape) for array in arrays]
    return call(body, held, [HBM] * len(held), shapes, [VMEM] * len(held), [pltpu.SemaphoreType.DMA((len(held),))])


def step(pieces, fields, cond, src, y_in, x_in, layers, z_spans, x_head, last, write=None):
    J, I, K, L = cond.shape
    nl = len(layers)
    z_ports, y_ports, x_ports = ports_of("cols"), ports_of("rows"), ports_of("slabs")
    first = pieces[0][1]
    rows = sum(piece[2] for piece in pieces)
    ins, slots = [], {}

    def add(array):
        if id(array) not in slots:
            slots[id(array)] = len(ins)
            ins.append(array)
        return slots[id(array)]

    cond_at, src_at = add(cond), add(src)
    near = {q + d for q, *_ in pieces for d in (-1, 0, 1)} & set(range(len(fields)))
    field_at = {q: add(fields[q][0]) for q in sorted(near)}
    z_at = [[add(array) for array in piece[3]] for piece in pieces]
    y_at = {q: [add(array) for array in y_in[q][0]] for q, *_ in pieces}
    x_at = [add(array) for array in x_in]
    head_at = add(x_head) if x_head is not None else None
    if write is not None:
        done, done_layers, (done_first, done_rows), buffer = write
        done_at = add(done)
        buffers = [] if buffer is None else [buffer]

    def body(*refs):
        if write is not None:
            copies = write_copies(refs[done_at], refs[-2], done_layers, done_first, done_rows, refs[-1])
            for copy in copies:
                copy.start()
            compute(refs[: len(ins)] + refs[len(ins) + len(buffers) : -2])
            for copy in copies:
                copy.wait()
        else:
            compute(refs)

    def compute(refs):
        outs = list(refs[len(ins) :])
        c, s = refs[cond_at], refs[src_at]
        out = outs.pop(0)
        if last:
            stats = outs.pop(0)
        else:
            z_out = [[outs.pop(0) for _ in z_ports] for _ in z_spans]
            y_out = [outs.pop(0) for _ in y_ports]
            x_out = [outs.pop(0) for _ in x_ports] if x_head is not None else []
        x_lo, x_hi = halo_readers("slabs", [refs[n] for n in x_at])
        sublane = lax.broadcasted_iota(jnp.int32, (ROWS, L), 0)

        def tile(k, q, z, z_first, z_to, z_to_first, at_low, at_high):
            u, base = refs[field_at[q]], fields[q][1]
            y_lo, y_hi = halo_readers("rows", [refs[n] for n in y_at[q]])
            if z:
                z_lo, z_hi = halo_readers("cols", z)
            in_y = pl.ds(k - y_in[q][1], ROWS)
            in_z = pl.ds(k - z_first, ROWS)
            here = pl.ds(k - first, ROWS)
            there = pl.ds(k, ROWS)
            known = {}

            def cells(j, i):
                if (j, i) not in known:
                    if j < 0:
                        known[j, i] = y_lo((i, in_y))
                    elif j >= J:
                        known[j, i] = y_hi((i, in_y))
                    elif i < 0:
                        known[j, i] = z_lo((j, in_z))
                    elif i >= I:
                        known[j, i] = z_hi((j, in_z))
                    else:
                        known[j, i] = u[j, i, pl.ds(k - base, ROWS)]
                return known[j, i]

            def edge_row(near_q, j, i, row):
                array, start = refs[field_at[near_q]], fields[near_q][1]
                return jnp.broadcast_to(array[j, i, pl.ds(row - start, 1)], (ROWS, L))

            def k_lower(j, i):
                if not at_low:
                    return u[j, i, pl.ds(k - base - 1, ROWS)]
                if q > 0:
                    edge = edge_row(q - 1, j, i, k - 1)
                else:
                    edge = jnp.broadcast_to(x_lo((j, pl.ds(i, 1))), (ROWS, L))
                return jnp.where(sublane == 0, edge, pltpu.roll(cells(j, i), 1, 0))

            def k_upper(j, i):
                if not at_high:
                    return u[j, i, pl.ds(k - base + 1, ROWS)]
                if q + 1 < len(fields):
                    edge = edge_row(q + 1, j, i, k + ROWS)
                else:
                    edge = jnp.broadcast_to(x_hi((j, pl.ds(i, 1))), (ROWS, L))
                return jnp.where(sublane == ROWS - 1, edge, pltpu.roll(cells(j, i), ROWS - 1, 0))

            totals = [None] * nl
            for j in range(J):
                for n, i in enumerate(layers):
                    middle = cells(j, i)
                    spread = (
                        (cells(j - 1, i) + cells(j + 1, i))
                        + (cells(j, i - 1) + cells(j, i + 1))
                        + (k_lower(j, i) + k_upper(j, i))
                        - 6.0 * middle
                    )
                    new = middle + c[j, i, there] * spread + s[j, i, there]
                    out[j, n, here] = new
                    if last:
                        totals[n] = new if j == 0 else totals[n] + new
                    if i == 0:
                        lowest = new
                    if i == I - 1:
                        highest = new
                if not last:
                    for ref, port in zip(z_to, z_ports):
                        ref[j, pl.ds(k - z_to_first, ROWS)] = jnp.where(is_upper("cols", port) == 1, lowest, highest)
                for at in list(known):
                    if at[0] < j:
                        del known[at]
            if last:
                for n in range(nl):
                    mean = totals[n] * (1.0 / J)
                    spread = None
                    for j in range(J):
                        off = out[j, n, here] - mean
                        spread = off * off if j == 0 else spread + off * off
                    stats[0, n, here] = mean
                    stats[1, n, here] = spread

        for (q, k0, kc, _), z_refs in zip(pieces, z_at):
            z = [refs[n] for n in z_refs]
            array_low, array_high = fields[q][1], fields[q][1] + fields[q][0].shape[2]
            targets = [(0, K, None)] if last else [(*span, n) for n, span in enumerate(z_spans)]
            for t0, tc, n in targets:
                low, high = max(k0, t0), min(k0 + kc, t0 + tc)
                if low >= high:
                    continue
                z_to = z_out[n] if n is not None else []
                same = (q, z, k0, z_to, t0)
                begin, end = low, high
                if low == array_low:
                    tile(low, *same, True, low + ROWS == array_high)
                    begin += ROWS
                if high == array_high and begin < high:
                    tile(high - ROWS, *same, False, True)
                    end -= ROWS
                if begin < end:

                    def inner(t, carry, same=same):
                        tile(pl.multiple_of(t * ROWS, ROWS), *same, False, False)
                        return carry

                    lax.fori_loop(begin // ROWS, end // ROWS, inner, 0)
        if not last:
            for ref, port in zip(y_out, y_ports):
                ref[...] = out[sent_index("rows", port, J)]
            for ref, port in zip(x_out, x_ports):
                for j in range(J):
                    head = refs[head_at][j, :, 0, :]
                    tail = out[j, :, rows - 1, :]
                    upper = is_upper("slabs", port).astype(F32)
                    ref[j] = head * upper + tail * (1.0 - upper)

    shapes = [vmem(J, nl, rows, L)]
    if last:
        shapes.append(vmem(2, nl, rows, L))
    else:
        for _, tc in z_spans:
            shapes += [vmem(J, tc, L)] * len(z_ports)
        shapes += [vmem(I, rows, L)] * len(y_ports)
        if x_head is not None:
            shapes += [vmem(J, I, L)] * len(x_ports)
    all_ins, in_specs, out_specs, scratch, aliases = ins, [VMEM] * len(ins), [VMEM] * len(shapes), [], None
    if write is not None:
        all_ins, in_specs = ins + buffers, in_specs + [HBM] * len(buffers)
        aliases = {len(ins): len(shapes)} if buffers else None
        shapes, out_specs = shapes + [jax.ShapeDtypeStruct(cond.shape, F32)], out_specs + [HBM]
        scratch = [pltpu.SemaphoreType.DMA((len(done_layers),))]
    outs = list(call(body, all_ins, in_specs, shapes, out_specs, scratch, aliases, flops=10 * J * nl * rows * L))
    new = outs.pop(0)
    if last:
        return new, outs[0], outs[1] if write is not None else None
    z = [[outs.pop(0) for _ in z_ports] for _ in z_spans]
    y = [outs.pop(0) for _ in y_ports]
    return new, z, y, outs


def finish(new, own, others, layers, span, anomaly, field, shape):
    J, _, _, L = shape
    k0, kc = span
    nl = len(layers)
    count = len(others) + 1
    buffers = [buffer for buffer in (anomaly, field) if buffer is not None]
    outs_count = 1 if field is None else 2

    def body(*refs):
        u, sums = refs[0], refs[1 : 1 + count]
        outs = refs[1 + count + len(buffers) : 1 + count + len(buffers) + outs_count]
        scaled, sems = refs[-2:]
        copies = []
        if field is not None:
            copies += write_copies(u, outs[1], layers, k0, kc, sems.at[1])
            for copy in copies:
                copy.start()
        results = write_copies(scaled, outs[0], layers, k0, kc, sems.at[0])
        for n in range(nl):

            def tile(t, carry, n=n):
                here = pl.ds(pl.multiple_of(t * ROWS, ROWS), ROWS)
                means = [ref[0, n, here] for ref in sums]
                mean = means[0]
                for other in means[1:]:
                    mean = mean + other
                mean = mean * (1.0 / count)
                spread = None
                for ref, own_mean in zip(sums, means):
                    off = own_mean - mean
                    part = ref[1, n, here] + J * (off * off)
                    spread = part if spread is None else spread + part
                scale = lax.rsqrt(spread * (1.0 / (J * count)) + 0.0001)
                for j in range(J):
                    scaled[j, n, here] = (u[j, n, here] - mean) * scale
                return carry

            lax.fori_loop(0, kc // ROWS, tile, 0)
            results[n].start()
        for copy in copies + results:
            copy.wait()

    ins = [new, own] + list(others)
    aliases = {len(ins) + n: (n if anomaly is not None else 1) for n in range(len(buffers))}
    return call(
        body,
        ins + buffers,
        [VMEM] * len(ins) + [HBM] * len(buffers),
        [jax.ShapeDtypeStruct(shape, F32)] * outs_count,
        [HBM] * outs_count,
        [pltpu.VMEM((J, nl, kc, L), F32), pltpu.SemaphoreType.DMA((2, nl))],
        aliases,
        flops=10 * J * nl * kc * L,
    )


def other_rows(own):
    count = lax.axis_size("rows")
    return [lax.ppermute(own, "rows", [(i, (i + shift) % count) for i in range(count)]) for shift in range(1, count)]


def spans_of(start, extent, weights):
    tiles, total, cuts = extent // ROWS, sum(weights), [0]
    for n in range(1, len(weights) + 1):
        cuts.append(round(tiles * sum(weights[:n]) / total))
    return [(start + a * ROWS, (b - a) * ROWS) for a, b in zip(cuts, cuts[1:]) if b > a]


def on_device(field_values, conductance, source):
    shape = J, I, K, L = field_values.shape
    spans = spans_of(0, K, CHUNKS)
    chunks = range(len(spans))

    def trade(z, y):
        z_got = []
        for faces in z:
            z_got.append(exchange(faces, "cols"))
        return z_got, exchange(y, "rows")

    z_out = cut_faces(field_values, spans[:1], [], False)[0]
    z_rest, y_out, x_out = cut_faces(field_values, spans[1:], spans, True)
    z_out += z_rest
    z_in, y_in = [], []
    for q in chunks:
        z_got, y_got = trade([z_out[q]], y_out[q])
        z_in.append([(*spans[q], z_got[0])])
        y_in.append((y_got, spans[q][0]))
    x_in = exchange(x_out, "slabs")
    staged, conductance, source = stage([field_values, conductance, source])
    fields = [(staged, 0) for _ in chunks]
    for step_no in range(1, STEPS):
        newer, z_next, y_next = [], [], []
        for q in chunks:
            is_end = q == len(spans) - 1
            z_spans = spans_of(*spans[q], LAST_CUT) if is_end and step_no == STEPS - 1 else [spans[q]]
            pieces = [(q, k0, kc, faces) for k0, kc, faces in z_in[q]]
            new, z, y, x_out = step(
                pieces,
                fields,
                conductance,
                source,
                y_in,
                x_in,
                range(I),
                z_spans,
                (newer + [(None, 0)])[0][0] if is_end else None,
                False,
            )
            newer.append((new, spans[q][0]))
            z_got, y_got = trade(z, y)
            z_next.append([(*span, faces) for span, faces in zip(z_spans, z_got)])
            y_next.append((y_got, spans[q][0]))
        x_in = exchange(x_out, "slabs")
        fields, z_in, y_in = newer, z_next, y_next

    inner, outer = list(range(1, I - 1)), [0, I - 1]
    jobs = []
    if inner:
        jobs.append((inner, [(q, *spans[q], []) for q in chunks]))
    for q in chunks:
        for k0, kc, faces in z_in[q]:
            jobs.append((outer, [(q, k0, kc, faces)]))
    anomaly, field, write, sums = None, None, None, []
    for n, (layers, pieces) in enumerate(jobs):
        new, own, wrote = step(pieces, fields, conductance, source, y_in, x_in, layers, [], None, True, write)
        field = field if wrote is None else wrote
        others = other_rows(own)
        span = (pieces[0][1], sum(piece[2] for piece in pieces))
        write = (new, layers, span, field) if n < len(jobs) - 2 else None
        sums.append((new, own, others, layers, span))
    for n, job in enumerate(sums):
        to_field = field if n >= len(sums) - 2 else None
        done = finish(*job, anomaly, to_field, shape)
        anomaly = done[0]
        field = done[1] if to_field is not None else field
    return anomaly, field


def solution(mesh):
    spec = P(("trial", "rows"), "cols", "slabs", None)

    return jax.shard_map(on_device, mesh=mesh, in_specs=(spec, spec, spec), out_specs=(spec, spec), check_vma=False)
```

```python
import jax
import jax.numpy as jnp
from jax import lax
from jax.experimental import pallas as pl
from jax.experimental.pallas import tpu as pltpu
from jax.sharding import PartitionSpec as P


STEPS = 4
CHUNKS = (11, 5)
LAST_CUT = (3, 2)
ROWS = 8
HBM = pl.BlockSpec(memory_space=pltpu.HBM)
VMEM = pl.BlockSpec(memory_space=pltpu.VMEM)
F32 = jnp.float32


def vmem(*shape):
    return pltpu.VMEM(shape, F32)


def call(body, ins, in_specs, outs, out_specs, scratch=(), aliases=None, flops=0):
    return pl.pallas_call(
        body,
        in_specs=in_specs,
        out_shape=outs,
        out_specs=out_specs,
        scratch_shapes=scratch,
        input_output_aliases=aliases or {},
        compiler_params=pltpu.CompilerParams(vmem_limit_bytes=12 * 2**20),
        cost_estimate=pl.CostEstimate(flops=flops, bytes_accessed=0, transcendentals=0) if flops else None,
    )(*ins)


def ports_of(axis):
    return (0,) if lax.axis_size(axis) == 2 else (0, 1)


def exchange(buffers, axis):
    count, trials = lax.axis_size(axis), lax.axis_size("trial")
    received = []
    for port, buffer in zip(ports_of(axis), buffers):
        pairs, alone = [], set(range(count))
        for i in range(port, count - 1, 2):
            pairs += [(i * trials + t, (i + 1) * trials + t) for t in range(trials)]
            alone -= {i, i + 1}
        pairs += [(i * trials + t, i * trials + t + 1) for i in sorted(alone) for t in range(0, trials - 1, 2)]
        received.append(lax.ppermute(buffer, (axis, "trial"), pairs + [(b, a) for a, b in pairs]))
    return received


def is_upper(axis, port):
    odd = lax.axis_index(axis) % 2
    return odd if port == 0 else 1 - odd


def sent_index(axis, port, extent):
    return (1 - is_upper(axis, port)) * (extent - 1)


def halo_readers(axis, refs):
    at, upper = lax.axis_index(axis), is_upper(axis, 0)
    has_lower = (at > 0).astype(F32)
    has_upper = (at < lax.axis_size(axis) - 1).astype(F32)
    if len(refs) == 1:
        return (lambda where: refs[0][where] * has_lower), (lambda where: refs[0][where] * has_upper)
    return (
        lambda where: jnp.where(upper == 1, refs[0][where], refs[1][where]) * has_lower,
        lambda where: jnp.where(upper == 1, refs[1][where], refs[0][where]) * has_upper,
    )


def run_copies(copies):
    for copy in copies:
        copy.start()
    for copy in copies:
        copy.wait()


def write_copies(cells, out, layers, first, rows, sems):
    return [
        pltpu.make_async_copy(cells.at[:, n], out.at[:, i, pl.ds(first, rows)], sems.at[n]) for n, i in enumerate(layers)
    ]


def cut_faces(field, z_spans, y_spans, with_x):
    J, I, K, L = field.shape
    z_ports, y_ports, x_ports = ports_of("cols"), ports_of("rows"), ports_of("slabs") if with_x else ()
    shapes = [vmem(J, kc, L) for _, kc in z_spans for _ in z_ports]
    shapes += [vmem(I, kc, L) for _, kc in y_spans for _ in y_ports]
    shapes += [vmem(J, I, L) for _ in x_ports]

    def body(u, *refs):
        sources = [u.at[:, sent_index("cols", port, I), pl.ds(k0, kc)] for k0, kc in z_spans for port in z_ports]
        sources += [u.at[sent_index("rows", port, J), :, pl.ds(k0, kc)] for k0, kc in y_spans for port in y_ports]
        sources += [u.at[:, :, sent_index("slabs", port, K)] for port in x_ports]
        run_copies([pltpu.make_async_copy(src, refs[n], refs[-1].at[n]) for n, src in enumerate(sources)])

    field = pltpu.with_memory_space_constraint(field, pltpu.HBM)
    outs = list(call(body, [field], [HBM], shapes, [VMEM] * len(shapes), [pltpu.SemaphoreType.DMA((len(shapes),))]))
    z = [[outs.pop(0) for _ in z_ports] for _ in z_spans]
    y = [[outs.pop(0) for _ in y_ports] for _ in y_spans]
    return z, y, outs


def stage(arrays):
    def body(*refs):
        n = len(arrays)
        run_copies([pltpu.make_async_copy(refs[m], refs[n + m], refs[-1].at[m]) for m in range(n)])

    held = [pltpu.with_memory_space_constraint(array, pltpu.HBM) for array in arrays]
    shapes = [vmem(*array.shape) for array in arrays]
    return call(body, held, [HBM] * len(held), shapes, [VMEM] * len(held), [pltpu.SemaphoreType.DMA((len(held),))])


def step(pieces, fields, cond, src, y_in, x_in, layers, z_spans, x_head, last, write=None):
    J, I, K, L = cond.shape
    nl = len(layers)
    z_ports, y_ports, x_ports = ports_of("cols"), ports_of("rows"), ports_of("slabs")
    first = pieces[0][1]
    rows = sum(piece[2] for piece in pieces)
    ins, slots = [], {}

    def add(array):
        if id(array) not in slots:
            slots[id(array)] = len(ins)
            ins.append(array)
        return slots[id(array)]

    cond_at, src_at = add(cond), add(src)
    near = {q + d for q, *_ in pieces for d in (-1, 0, 1)} & set(range(len(fields)))
    field_at = {q: add(fields[q][0]) for q in sorted(near)}
    z_at = [[add(array) for array in piece[3]] for piece in pieces]
    y_at = {q: [add(array) for array in y_in[q][0]] for q, *_ in pieces}
    x_at = [add(array) for array in x_in]
    head_at = add(x_head) if x_head is not None else None
    if write is not None:
        done, done_layers, (done_first, done_rows), buffer = write
        done_at = add(done)
        buffers = [] if buffer is None else [buffer]

    def body(*refs):
        if write is not None:
            copies = write_copies(refs[done_at], refs[-2], done_layers, done_first, done_rows, refs[-1])
            for copy in copies:
                copy.start()
            compute(refs[: len(ins)] + refs[len(ins) + len(buffers) : -2])
            for copy in copies:
                copy.wait()
        else:
            compute(refs)

    def compute(refs):
        outs = list(refs[len(ins) :])
        c, s = refs[cond_at], refs[src_at]
        out = outs.pop(0)
        if last:
            stats = outs.pop(0)
        else:
            z_out = [[outs.pop(0) for _ in z_ports] for _ in z_spans]
            y_out = [outs.pop(0) for _ in y_ports]
            x_out = [outs.pop(0) for _ in x_ports] if x_head is not None else []
        x_lo, x_hi = halo_readers("slabs", [refs[n] for n in x_at])
        sublane = lax.broadcasted_iota(jnp.int32, (ROWS, L), 0)

        def tile(k, q, z, z_first, z_to, z_to_first, at_low, at_high):
            u, base = refs[field_at[q]], fields[q][1]
            y_lo, y_hi = halo_readers("rows", [refs[n] for n in y_at[q]])
            if z:
                z_lo, z_hi = halo_readers("cols", z)
            in_y = pl.ds(k - y_in[q][1], ROWS)
            in_z = pl.ds(k - z_first, ROWS)
            here = pl.ds(k - first, ROWS)
            there = pl.ds(k, ROWS)
            known = {}

            def cells(j, i):
                if (j, i) not in known:
                    if j < 0:
                        known[j, i] = y_lo((i, in_y))
                    elif j >= J:
                        known[j, i] = y_hi((i, in_y))
                    elif i < 0:
                        known[j, i] = z_lo((j, in_z))
                    elif i >= I:
                        known[j, i] = z_hi((j, in_z))
                    else:
                        known[j, i] = u[j, i, pl.ds(k - base, ROWS)]
                return known[j, i]

            def edge_row(near_q, j, i, row):
                array, start = refs[field_at[near_q]], fields[near_q][1]
                return jnp.broadcast_to(array[j, i, pl.ds(row - start, 1)], (ROWS, L))

            def k_lower(j, i):
                if not at_low:
                    return u[j, i, pl.ds(k - base - 1, ROWS)]
                if q > 0:
                    edge = edge_row(q - 1, j, i, k - 1)
                else:
                    edge = jnp.broadcast_to(x_lo((j, pl.ds(i, 1))), (ROWS, L))
                return jnp.where(sublane == 0, edge, pltpu.roll(cells(j, i), 1, 0))

            def k_upper(j, i):
                if not at_high:
                    return u[j, i, pl.ds(k - base + 1, ROWS)]
                if q + 1 < len(fields):
                    edge = edge_row(q + 1, j, i, k + ROWS)
                else:
                    edge = jnp.broadcast_to(x_hi((j, pl.ds(i, 1))), (ROWS, L))
                return jnp.where(sublane == ROWS - 1, edge, pltpu.roll(cells(j, i), ROWS - 1, 0))

            totals = [None] * nl
            for j in range(J):
                for n, i in enumerate(layers):
                    middle = cells(j, i)
                    spread = (
                        (cells(j - 1, i) + cells(j + 1, i))
                        + (cells(j, i - 1) + cells(j, i + 1))
                        + (k_lower(j, i) + k_upper(j, i))
                        - 6.0 * middle
                    )
                    new = middle + c[j, i, there] * spread + s[j, i, there]
                    out[j, n, here] = new
                    if last:
                        totals[n] = new if j == 0 else totals[n] + new
                    if i == 0:
                        lowest = new
                    if i == I - 1:
                        highest = new
                if not last:
                    for ref, port in zip(z_to, z_ports):
                        ref[j, pl.ds(k - z_to_first, ROWS)] = jnp.where(is_upper("cols", port) == 1, lowest, highest)
                for at in list(known):
                    if at[0] < j:
                        del known[at]
            if last:
                for n in range(nl):
                    mean = totals[n] * (1.0 / J)
                    spread = None
                    for j in range(J):
                        off = out[j, n, here] - mean
                        spread = off * off if j == 0 else spread + off * off
                    stats[0, n, here] = mean
                    stats[1, n, here] = spread

        for (q, k0, kc, _), z_refs in zip(pieces, z_at):
            z = [refs[n] for n in z_refs]
            array_low, array_high = fields[q][1], fields[q][1] + fields[q][0].shape[2]
            targets = [(0, K, None)] if last else [(*span, n) for n, span in enumerate(z_spans)]
            for t0, tc, n in targets:
                low, high = max(k0, t0), min(k0 + kc, t0 + tc)
                if low >= high:
                    continue
                z_to = z_out[n] if n is not None else []
                same = (q, z, k0, z_to, t0)
                begin, end = low, high
                if low == array_low:
                    tile(low, *same, True, low + ROWS == array_high)
                    begin += ROWS
                if high == array_high and begin < high:
                    tile(high - ROWS, *same, False, True)
                    end -= ROWS
                if begin < end:

                    def inner(t, carry, same=same):
                        tile(pl.multiple_of(t * ROWS, ROWS), *same, False, False)
                        return carry

                    lax.fori_loop(begin // ROWS, end // ROWS, inner, 0)
        if not last:
            for ref, port in zip(y_out, y_ports):
                ref[...] = out[sent_index("rows", port, J)]
            for ref, port in zip(x_out, x_ports):
                for j in range(J):
                    head = refs[head_at][j, :, 0, :]
                    tail = out[j, :, rows - 1, :]
                    upper = is_upper("slabs", port).astype(F32)
                    ref[j] = head * upper + tail * (1.0 - upper)

    shapes = [vmem(J, nl, rows, L)]
    if last:
        shapes.append(vmem(2, nl, rows, L))
    else:
        for _, tc in z_spans:
            shapes += [vmem(J, tc, L)] * len(z_ports)
        shapes += [vmem(I, rows, L)] * len(y_ports)
        if x_head is not None:
            shapes += [vmem(J, I, L)] * len(x_ports)
    all_ins, in_specs, out_specs, scratch, aliases = ins, [VMEM] * len(ins), [VMEM] * len(shapes), [], None
    if write is not None:
        all_ins, in_specs = ins + buffers, in_specs + [HBM] * len(buffers)
        aliases = {len(ins): len(shapes)} if buffers else None
        shapes, out_specs = shapes + [jax.ShapeDtypeStruct(cond.shape, F32)], out_specs + [HBM]
        scratch = [pltpu.SemaphoreType.DMA((len(done_layers),))]
    outs = list(call(body, all_ins, in_specs, shapes, out_specs, scratch, aliases, flops=10 * J * nl * rows * L))
    new = outs.pop(0)
    if last:
        return new, outs[0], outs[1] if write is not None else None
    z = [[outs.pop(0) for _ in z_ports] for _ in z_spans]
    y = [outs.pop(0) for _ in y_ports]
    return new, z, y, outs


def finish(jobs, anomaly, field, shape):
    J, _, _, L = shape
    buffers = [buffer for buffer in (anomaly, field) if buffer is not None]
    outs_count = 1 if field is None else 2
    ins, scratch = [], []
    for new, own, others, layers, (k0, kc) in jobs:
        ins += [new, own] + list(others)
        scratch += [pltpu.VMEM((J, len(layers), kc, L), F32), pltpu.SemaphoreType.DMA((2, len(layers)))]

    def body(*refs):
        refs = list(refs)
        cells = []
        for _, _, others, _, _ in jobs:
            cells.append((refs.pop(0), [refs.pop(0) for _ in range(1 + len(others))]))
        for _ in buffers:
            refs.pop(0)
        outs = [refs.pop(0) for _ in range(outs_count)]
        copies = []
        if field is not None:
            for n, ((u, _), (*_, layers, (k0, kc))) in enumerate(zip(cells, jobs)):
                copies += write_copies(u, outs[1], layers, k0, kc, refs[2 * n + 1].at[1])
            for copy in copies:
                copy.start()
        for m, ((u, sums), (*_, layers, (k0, kc))) in enumerate(zip(cells, jobs)):
            scaled, sems = refs[2 * m], refs[2 * m + 1]
            results = write_copies(scaled, outs[0], layers, k0, kc, sems.at[0])
            for n in range(len(layers)):

                def tile(t, carry, n=n, u=u, sums=sums, scaled=scaled):
                    here = pl.ds(pl.multiple_of(t * ROWS, ROWS), ROWS)
                    count = len(sums)
                    means = [ref[0, n, here] for ref in sums]
                    mean = means[0]
                    for other in means[1:]:
                        mean = mean + other
                    mean = mean * (1.0 / count)
                    spread = None
                    for ref, own_mean in zip(sums, means):
                        off = own_mean - mean
                        part = ref[1, n, here] + J * (off * off)
                        spread = part if spread is None else spread + part
                    scale = lax.rsqrt(spread * (1.0 / (J * count)) + 0.0001)
                    for j in range(J):
                        scaled[j, n, here] = (u[j, n, here] - mean) * scale
                    return carry

                lax.fori_loop(0, kc // ROWS, tile, 0)
                results[n].start()
            copies += results
        for copy in copies:
            copy.wait()

    aliases = {len(ins) + n: (n if anomaly is not None else 1) for n in range(len(buffers))}
    return call(
        body,
        ins + buffers,
        [VMEM] * len(ins) + [HBM] * len(buffers),
        [jax.ShapeDtypeStruct(shape, F32)] * outs_count,
        [HBM] * outs_count,
        scratch,
        aliases,
        flops=sum(10 * J * len(layers) * kc * L for *_, layers, (_, kc) in jobs),
    )


def other_rows(own):
    count = lax.axis_size("rows")
    return [lax.ppermute(own, "rows", [(i, (i + shift) % count) for i in range(count)]) for shift in range(1, count)]


def spans_of(start, extent, weights):
    tiles, total, cuts = extent // ROWS, sum(weights), [0]
    for n in range(1, len(weights) + 1):
        cuts.append(round(tiles * sum(weights[:n]) / total))
    return [(start + a * ROWS, (b - a) * ROWS) for a, b in zip(cuts, cuts[1:]) if b > a]


def on_device(field_values, conductance, source):
    shape = J, I, K, L = field_values.shape
    spans = spans_of(0, K, CHUNKS)
    chunks = range(len(spans))

    def trade(z, y):
        z_got = []
        for faces in z:
            z_got.append(exchange(faces, "cols"))
        return z_got, exchange(y, "rows")

    z_out = cut_faces(field_values, spans[:1], [], False)[0]
    z_rest, y_out, x_out = cut_faces(field_values, spans[1:], spans, True)
    z_out += z_rest
    z_in, y_in = [], []
    for q in chunks:
        z_got, y_got = trade([z_out[q]], y_out[q])
        z_in.append([(*spans[q], z_got[0])])
        y_in.append((y_got, spans[q][0]))
    x_in = exchange(x_out, "slabs")
    staged, conductance, source = stage([field_values, conductance, source])
    fields = [(staged, 0) for _ in chunks]
    for step_no in range(1, STEPS):
        newer, z_next, y_next = [], [], []
        for q in chunks:
            is_end = q == len(spans) - 1
            z_spans = spans_of(*spans[q], LAST_CUT) if is_end and step_no == STEPS - 1 else [spans[q]]
            pieces = [(q, k0, kc, faces) for k0, kc, faces in z_in[q]]
            new, z, y, x_out = step(
                pieces,
                fields,
                conductance,
                source,
                y_in,
                x_in,
                range(I),
                z_spans,
                (newer + [(None, 0)])[0][0] if is_end else None,
                False,
            )
            newer.append((new, spans[q][0]))
            z_got, y_got = trade(z, y)
            z_next.append([(*span, faces) for span, faces in zip(z_spans, z_got)])
            y_next.append((y_got, spans[q][0]))
        x_in = exchange(x_out, "slabs")
        fields, z_in, y_in = newer, z_next, y_next

    inner, outer = list(range(1, I - 1)), [0, I - 1]
    jobs = []
    if inner:
        jobs.append((inner, [(q, *spans[q], []) for q in chunks]))
    for q in chunks:
        for k0, kc, faces in z_in[q]:
            jobs.append((outer, [(q, k0, kc, faces)]))
    anomaly, field, write, sums = None, None, None, []
    for n, (layers, pieces) in enumerate(jobs):
        new, own, wrote = step(pieces, fields, conductance, source, y_in, x_in, layers, [], None, True, write)
        field = field if wrote is None else wrote
        others = other_rows(own)
        span = (pieces[0][1], sum(piece[2] for piece in pieces))
        write = (new, layers, span, field) if n == 0 else None
        sums.append((new, own, others, layers, span))
    for n, group in enumerate(([sums[0]], [sums[1]], sums[2:])):
        if group:
            done = finish(group, anomaly, field if n > 0 else None, shape)
            anomaly = done[0]
            field = done[1] if n > 0 else field
    return anomaly, field


def solution(mesh):
    spec = P(("trial", "rows"), "cols", "slabs", None)

    return jax.shard_map(on_device, mesh=mesh, in_specs=(spec, spec, spec), out_specs=(spec, spec), check_vma=False)
```

```python
import jax
import jax.numpy as jnp
from jax import lax
from jax.experimental import pallas as pl
from jax.experimental.pallas import tpu as pltpu
from jax.sharding import PartitionSpec as P


STEPS = 4
CHUNKS = (11, 5)
LAST_CUT = (4, 1)
ROWS = 8
HBM = pl.BlockSpec(memory_space=pltpu.HBM)
VMEM = pl.BlockSpec(memory_space=pltpu.VMEM)
F32 = jnp.float32


def vmem(*shape):
    return pltpu.VMEM(shape, F32)


def call(body, ins, in_specs, outs, out_specs, scratch=(), aliases=None, flops=0):
    return pl.pallas_call(
        body,
        in_specs=in_specs,
        out_shape=outs,
        out_specs=out_specs,
        scratch_shapes=scratch,
        input_output_aliases=aliases or {},
        compiler_params=pltpu.CompilerParams(vmem_limit_bytes=12 * 2**20),
        cost_estimate=pl.CostEstimate(flops=flops, bytes_accessed=0, transcendentals=0) if flops else None,
    )(*ins)


def ports_of(axis):
    return (0,) if lax.axis_size(axis) == 2 else (0, 1)


def exchange(buffers, axis):
    count, trials = lax.axis_size(axis), lax.axis_size("trial")
    received = []
    for port, buffer in zip(ports_of(axis), buffers):
        pairs, alone = [], set(range(count))
        for i in range(port, count - 1, 2):
            pairs += [(i * trials + t, (i + 1) * trials + t) for t in range(trials)]
            alone -= {i, i + 1}
        pairs += [(i * trials + t, i * trials + t + 1) for i in sorted(alone) for t in range(0, trials - 1, 2)]
        received.append(lax.ppermute(buffer, (axis, "trial"), pairs + [(b, a) for a, b in pairs]))
    return received


def is_upper(axis, port):
    odd = lax.axis_index(axis) % 2
    return odd if port == 0 else 1 - odd


def sent_index(axis, port, extent):
    return (1 - is_upper(axis, port)) * (extent - 1)


def halo_readers(axis, refs):
    at, upper = lax.axis_index(axis), is_upper(axis, 0)
    has_lower = (at > 0).astype(F32)
    has_upper = (at < lax.axis_size(axis) - 1).astype(F32)
    if len(refs) == 1:
        return (lambda where: refs[0][where] * has_lower), (lambda where: refs[0][where] * has_upper)
    return (
        lambda where: jnp.where(upper == 1, refs[0][where], refs[1][where]) * has_lower,
        lambda where: jnp.where(upper == 1, refs[1][where], refs[0][where]) * has_upper,
    )


def run_copies(copies):
    for copy in copies:
        copy.start()
    for copy in copies:
        copy.wait()


def write_copies(cells, out, layers, first, rows, sems):
    return [
        pltpu.make_async_copy(cells.at[:, n], out.at[:, i, pl.ds(first, rows)], sems.at[n]) for n, i in enumerate(layers)
    ]


def cut_faces(field, z_spans, y_spans, with_x):
    J, I, K, L = field.shape
    z_ports, y_ports, x_ports = ports_of("cols"), ports_of("rows"), ports_of("slabs") if with_x else ()
    shapes = [vmem(J, kc, L) for _, kc in z_spans for _ in z_ports]
    shapes += [vmem(I, kc, L) for _, kc in y_spans for _ in y_ports]
    shapes += [vmem(J, I, L) for _ in x_ports]

    def body(u, *refs):
        sources = [u.at[:, sent_index("cols", port, I), pl.ds(k0, kc)] for k0, kc in z_spans for port in z_ports]
        sources += [u.at[sent_index("rows", port, J), :, pl.ds(k0, kc)] for k0, kc in y_spans for port in y_ports]
        sources += [u.at[:, :, sent_index("slabs", port, K)] for port in x_ports]
        run_copies([pltpu.make_async_copy(src, refs[n], refs[-1].at[n]) for n, src in enumerate(sources)])

    field = pltpu.with_memory_space_constraint(field, pltpu.HBM)
    outs = list(call(body, [field], [HBM], shapes, [VMEM] * len(shapes), [pltpu.SemaphoreType.DMA((len(shapes),))]))
    z = [[outs.pop(0) for _ in z_ports] for _ in z_spans]
    y = [[outs.pop(0) for _ in y_ports] for _ in y_spans]
    return z, y, outs


def stage(arrays):
    def body(*refs):
        n = len(arrays)
        run_copies([pltpu.make_async_copy(refs[m], refs[n + m], refs[-1].at[m]) for m in range(n)])

    held = [pltpu.with_memory_space_constraint(array, pltpu.HBM) for array in arrays]
    shapes = [vmem(*array.shape) for array in arrays]
    return call(body, held, [HBM] * len(held), shapes, [VMEM] * len(held), [pltpu.SemaphoreType.DMA((len(held),))])


def step(pieces, fields, cond, src, y_in, x_in, layers, z_spans, x_head, last, write=None):
    J, I, K, L = cond.shape
    nl = len(layers)
    z_ports, y_ports, x_ports = ports_of("cols"), ports_of("rows"), ports_of("slabs")
    first = pieces[0][1]
    rows = sum(piece[2] for piece in pieces)
    ins, slots = [], {}

    def add(array):
        if id(array) not in slots:
            slots[id(array)] = len(ins)
            ins.append(array)
        return slots[id(array)]

    cond_at, src_at = add(cond), add(src)
    near = {q + d for q, *_ in pieces for d in (-1, 0, 1)} & set(range(len(fields)))
    field_at = {q: add(fields[q][0]) for q in sorted(near)}
    z_at = [[add(array) for array in piece[3]] for piece in pieces]
    y_at = {q: [add(array) for array in y_in[q][0]] for q, *_ in pieces}
    x_at = [add(array) for array in x_in]
    head_at = add(x_head) if x_head is not None else None
    if write is not None:
        done, done_layers, (done_first, done_rows), buffer = write
        done_at = add(done)
        buffers = [] if buffer is None else [buffer]

    def body(*refs):
        if write is not None:
            copies = write_copies(refs[done_at], refs[-2], done_layers, done_first, done_rows, refs[-1])
            for copy in copies:
                copy.start()
            compute(refs[: len(ins)] + refs[len(ins) + len(buffers) : -2])
            for copy in copies:
                copy.wait()
        else:
            compute(refs)

    def compute(refs):
        outs = list(refs[len(ins) :])
        c, s = refs[cond_at], refs[src_at]
        out = outs.pop(0)
        if last:
            stats = outs.pop(0)
        else:
            z_out = [[outs.pop(0) for _ in z_ports] for _ in z_spans]
            y_out = [outs.pop(0) for _ in y_ports]
            x_out = [outs.pop(0) for _ in x_ports] if x_head is not None else []
        x_lo, x_hi = halo_readers("slabs", [refs[n] for n in x_at])
        sublane = lax.broadcasted_iota(jnp.int32, (ROWS, L), 0)

        def tile(k, q, z, z_first, z_to, z_to_first, at_low, at_high):
            u, base = refs[field_at[q]], fields[q][1]
            y_lo, y_hi = halo_readers("rows", [refs[n] for n in y_at[q]])
            if z:
                z_lo, z_hi = halo_readers("cols", z)
            in_y = pl.ds(k - y_in[q][1], ROWS)
            in_z = pl.ds(k - z_first, ROWS)
            here = pl.ds(k - first, ROWS)
            there = pl.ds(k, ROWS)
            known = {}

            def cells(j, i):
                if (j, i) not in known:
                    if j < 0:
                        known[j, i] = y_lo((i, in_y))
                    elif j >= J:
                        known[j, i] = y_hi((i, in_y))
                    elif i < 0:
                        known[j, i] = z_lo((j, in_z))
                    elif i >= I:
                        known[j, i] = z_hi((j, in_z))
                    else:
                        known[j, i] = u[j, i, pl.ds(k - base, ROWS)]
                return known[j, i]

            def edge_row(near_q, j, i, row):
                array, start = refs[field_at[near_q]], fields[near_q][1]
                return jnp.broadcast_to(array[j, i, pl.ds(row - start, 1)], (ROWS, L))

            def k_lower(j, i):
                if not at_low:
                    return u[j, i, pl.ds(k - base - 1, ROWS)]
                if q > 0:
                    edge = edge_row(q - 1, j, i, k - 1)
                else:
                    edge = jnp.broadcast_to(x_lo((j, pl.ds(i, 1))), (ROWS, L))
                return jnp.where(sublane == 0, edge, pltpu.roll(cells(j, i), 1, 0))

            def k_upper(j, i):
                if not at_high:
                    return u[j, i, pl.ds(k - base + 1, ROWS)]
                if q + 1 < len(fields):
                    edge = edge_row(q + 1, j, i, k + ROWS)
                else:
                    edge = jnp.broadcast_to(x_hi((j, pl.ds(i, 1))), (ROWS, L))
                return jnp.where(sublane == ROWS - 1, edge, pltpu.roll(cells(j, i), ROWS - 1, 0))

            totals = [None] * nl
            for j in range(J):
                for n, i in enumerate(layers):
                    middle = cells(j, i)
                    spread = (
                        (cells(j - 1, i) + cells(j + 1, i))
                        + (cells(j, i - 1) + cells(j, i + 1))
                        + (k_lower(j, i) + k_upper(j, i))
                        - 6.0 * middle
                    )
                    new = middle + c[j, i, there] * spread + s[j, i, there]
                    out[j, n, here] = new
                    if last:
                        totals[n] = new if j == 0 else totals[n] + new
                    if i == 0:
                        lowest = new
                    if i == I - 1:
                        highest = new
                if not last:
                    for ref, port in zip(z_to, z_ports):
                        ref[j, pl.ds(k - z_to_first, ROWS)] = jnp.where(is_upper("cols", port) == 1, lowest, highest)
                for at in list(known):
                    if at[0] < j:
                        del known[at]
            if last:
                for n in range(nl):
                    mean = totals[n] * (1.0 / J)
                    spread = None
                    for j in range(J):
                        off = out[j, n, here] - mean
                        spread = off * off if j == 0 else spread + off * off
                    stats[0, n, here] = mean
                    stats[1, n, here] = spread

        for (q, k0, kc, _), z_refs in zip(pieces, z_at):
            z = [refs[n] for n in z_refs]
            array_low, array_high = fields[q][1], fields[q][1] + fields[q][0].shape[2]
            targets = [(0, K, None)] if last else [(*span, n) for n, span in enumerate(z_spans)]
            for t0, tc, n in targets:
                low, high = max(k0, t0), min(k0 + kc, t0 + tc)
                if low >= high:
                    continue
                z_to = z_out[n] if n is not None else []
                same = (q, z, k0, z_to, t0)
                begin, end = low, high
                if low == array_low:
                    tile(low, *same, True, low + ROWS == array_high)
                    begin += ROWS
                if high == array_high and begin < high:
                    tile(high - ROWS, *same, False, True)
                    end -= ROWS
                if begin < end:

                    def inner(t, carry, same=same):
                        tile(pl.multiple_of(t * ROWS, ROWS), *same, False, False)
                        return carry

                    lax.fori_loop(begin // ROWS, end // ROWS, inner, 0)
        if not last:
            for ref, port in zip(y_out, y_ports):
                ref[...] = out[sent_index("rows", port, J)]
            for ref, port in zip(x_out, x_ports):
                for j in range(J):
                    head = refs[head_at][j, :, 0, :]
                    tail = out[j, :, rows - 1, :]
                    upper = is_upper("slabs", port).astype(F32)
                    ref[j] = head * upper + tail * (1.0 - upper)

    shapes = [vmem(J, nl, rows, L)]
    if last:
        shapes.append(vmem(2, nl, rows, L))
    else:
        for _, tc in z_spans:
            shapes += [vmem(J, tc, L)] * len(z_ports)
        shapes += [vmem(I, rows, L)] * len(y_ports)
        if x_head is not None:
            shapes += [vmem(J, I, L)] * len(x_ports)
    all_ins, in_specs, out_specs, scratch, aliases = ins, [VMEM] * len(ins), [VMEM] * len(shapes), [], None
    if write is not None:
        all_ins, in_specs = ins + buffers, in_specs + [HBM] * len(buffers)
        aliases = {len(ins): len(shapes)} if buffers else None
        shapes, out_specs = shapes + [jax.ShapeDtypeStruct(cond.shape, F32)], out_specs + [HBM]
        scratch = [pltpu.SemaphoreType.DMA((len(done_layers),))]
    outs = list(call(body, all_ins, in_specs, shapes, out_specs, scratch, aliases, flops=10 * J * nl * rows * L))
    new = outs.pop(0)
    if last:
        return new, outs[0], outs[1] if write is not None else None
    z = [[outs.pop(0) for _ in z_ports] for _ in z_spans]
    y = [outs.pop(0) for _ in y_ports]
    return new, z, y, outs


def finish(jobs, finished, anomaly, field, shape):
    J, _, _, L = shape
    buffers = [buffer for buffer in (anomaly, field) if buffer is not None]
    outs_count = 1 if field is None else 2
    ins, scratch = [], []
    for new, own, others, layers, (k0, kc) in jobs:
        ins += [new, own] + list(others)
        scratch += [pltpu.VMEM((J, len(layers), kc, L), F32), pltpu.SemaphoreType.DMA((len(layers),))]
    ins += [job[0] for job in finished]
    scratch += [pltpu.SemaphoreType.DMA((len(job[3]),)) for job in finished]

    def body(*refs):
        refs = list(refs)
        cells = []
        for _, _, others, _, _ in jobs:
            cells.append((refs.pop(0), [refs.pop(0) for _ in range(1 + len(others))]))
        written = [refs.pop(0) for _ in finished]
        for _ in buffers:
            refs.pop(0)
        outs = [refs.pop(0) for _ in range(outs_count)]
        copies = []
        for n, (u, (*_, layers, (k0, kc))) in enumerate(zip(written, finished)):
            copies += write_copies(u, outs[1], layers, k0, kc, refs[2 * len(jobs) + n])
        for copy in copies:
            copy.start()
        for m, ((u, sums), (*_, layers, (k0, kc))) in enumerate(zip(cells, jobs)):
            scaled, sems = refs[2 * m], refs[2 * m + 1]
            results = write_copies(scaled, outs[0], layers, k0, kc, sems)
            for n in range(len(layers)):

                def tile(t, carry, n=n, u=u, sums=sums, scaled=scaled):
                    here = pl.ds(pl.multiple_of(t * ROWS, ROWS), ROWS)
                    count = len(sums)
                    means = [ref[0, n, here] for ref in sums]
                    mean = means[0]
                    for other in means[1:]:
                        mean = mean + other
                    mean = mean * (1.0 / count)
                    spread = None
                    for ref, own_mean in zip(sums, means):
                        off = own_mean - mean
                        part = ref[1, n, here] + J * (off * off)
                        spread = part if spread is None else spread + part
                    scale = lax.rsqrt(spread * (1.0 / (J * count)) + 0.0001)
                    for j in range(J):
                        scaled[j, n, here] = (u[j, n, here] - mean) * scale
                    return carry

                lax.fori_loop(0, kc // ROWS, tile, 0)
                results[n].start()
            copies += results
        for copy in copies:
            copy.wait()

    aliases = {len(ins) + n: (n if anomaly is not None else 1) for n in range(len(buffers))}
    return call(
        body,
        ins + buffers,
        [VMEM] * len(ins) + [HBM] * len(buffers),
        [jax.ShapeDtypeStruct(shape, F32)] * outs_count,
        [HBM] * outs_count,
        scratch,
        aliases,
        flops=sum(10 * J * len(layers) * kc * L for *_, layers, (_, kc) in jobs),
    )


def other_rows(own):
    count = lax.axis_size("rows")
    return [lax.ppermute(own, "rows", [(i, (i + shift) % count) for i in range(count)]) for shift in range(1, count)]


def spans_of(start, extent, weights):
    tiles, total, cuts = extent // ROWS, sum(weights), [0]
    for n in range(1, len(weights) + 1):
        cuts.append(round(tiles * sum(weights[:n]) / total))
    return [(start + a * ROWS, (b - a) * ROWS) for a, b in zip(cuts, cuts[1:]) if b > a]


def on_device(field_values, conductance, source):
    shape = J, I, K, L = field_values.shape
    spans = spans_of(0, K, CHUNKS)
    chunks = range(len(spans))

    def trade(z, y):
        z_got = []
        for faces in z:
            z_got.append(exchange(faces, "cols"))
        return z_got, exchange(y, "rows")

    z_out = cut_faces(field_values, spans[:1], [], False)[0]
    z_rest, y_out, x_out = cut_faces(field_values, spans[1:], spans, True)
    z_out += z_rest
    z_in, y_in = [], []
    for q in chunks:
        z_got, y_got = trade([z_out[q]], y_out[q])
        z_in.append([(*spans[q], z_got[0])])
        y_in.append((y_got, spans[q][0]))
    x_in = exchange(x_out, "slabs")
    staged, conductance, source = stage([field_values, conductance, source])
    fields = [(staged, 0) for _ in chunks]
    for step_no in range(1, STEPS):
        newer, z_next, y_next = [], [], []
        for q in chunks:
            is_end = q == len(spans) - 1
            z_spans = spans_of(*spans[q], LAST_CUT) if is_end and step_no == STEPS - 1 else [spans[q]]
            pieces = [(q, k0, kc, faces) for k0, kc, faces in z_in[q]]
            new, z, y, x_out = step(
                pieces,
                fields,
                conductance,
                source,
                y_in,
                x_in,
                range(I),
                z_spans,
                (newer + [(None, 0)])[0][0] if is_end else None,
                False,
            )
            newer.append((new, spans[q][0]))
            z_got, y_got = trade(z, y)
            z_next.append([(*span, faces) for span, faces in zip(z_spans, z_got)])
            y_next.append((y_got, spans[q][0]))
        x_in = exchange(x_out, "slabs")
        fields, z_in, y_in = newer, z_next, y_next

    inner, outer = list(range(1, I - 1)), [0, I - 1]
    jobs = []
    if inner:
        jobs.append((inner, [(q, *spans[q], []) for q in chunks]))
    for q in chunks:
        for k0, kc, faces in z_in[q]:
            jobs.append((outer, [(q, k0, kc, faces)]))
    anomaly, field, write, sums = None, None, None, []
    for n, (layers, pieces) in enumerate(jobs):
        new, own, wrote = step(pieces, fields, conductance, source, y_in, x_in, layers, [], None, True, write)
        field = field if wrote is None else wrote
        others = other_rows(own)
        span = (pieces[0][1], sum(piece[2] for piece in pieces))
        write = (new, layers, span, field) if n == 0 else None
        sums.append((new, own, others, layers, span))
    for n, group in enumerate(([sums[0]], [sums[1]], sums[2:])):
        if group:
            finished = sums[1:] if n == 1 else []
            done = finish(group, finished, anomaly, field if finished else None, shape)
            anomaly = done[0]
            field = done[1] if finished else field
    return anomaly, field


def solution(mesh):
    spec = P(("trial", "rows"), "cols", "slabs", None)

    return jax.shard_map(on_device, mesh=mesh, in_specs=(spec, spec, spec), out_specs=(spec, spec), check_vma=False)
```
